32 devices in a mesh: ep: 4 (over z), fsdp: 8 (over y, x, core).
Axes of the slice: x: 2, y: 2, z: 4, core: 2. Of those that a mesh axis runs over, the one named last changes fastest.
Arguments:
- x_in: bfloat16 [32, 512, 768], P(('ep', 'fsdp'))
- grad_y: bfloat16 [32, 512, 768], P(('ep', 'fsdp'))
- w_q: bfloat16 [768, 12, 64], P(('ep', 'fsdp'))
- w_k: bfloat16 [768, 12, 64], P(('ep', 'fsdp'))
- w_v: bfloat16 [768, 12, 64], P(('ep', 'fsdp'))
- w_o: bfloat16 [12, 64, 768], P(None, None, ('ep', 'fsdp'))
- gamma_attn: bfloat16 [768], P(('ep', 'fsdp'))
- gamma_mlp: bfloat16 [768], P(('ep', 'fsdp'))
- w_router: float32 [768, 8], P(('ep', 'fsdp'))
- w1_shared: bfloat16 [768, 3072], P(('ep', 'fsdp'))
- w3_shared: bfloat16 [768, 3072], P(('ep', 'fsdp'))
- w2_shared: bfloat16 [3072, 768], P(None, ('ep', 'fsdp'))
- w1_expert: bfloat16 [8, 768, 3072], P('ep', 'fsdp')
- w3_expert: bfloat16 [8, 768, 3072], P('ep', 'fsdp')
- w2_expert: bfloat16 [8, 3072, 768], P('ep', 'fsdp')
- expert_ids: int32 [32, 512], P(('ep', 'fsdp'))
Outputs:
- output 1: bfloat16 [32, 512, 768], P(('ep', 'fsdp'))
- output 2: bfloat16 [32, 512, 768], P(('ep', 'fsdp'))
- output 3: float32 [768, 12, 64], P(('ep', 'fsdp'))
- output 4: float32 [768, 12, 64], P(('ep', 'fsdp'))
- output 5: float32 [768, 12, 64], P(('ep', 'fsdp'))
- output 6: float32 [12, 64, 768], P(None, None, ('ep', 'fsdp'))
- output 7: float32 [768], P(('ep', 'fsdp'))
- output 8: float32 [768], P(('ep', 'fsdp'))
- output 9: float32 [768, 8], P(('ep', 'fsdp'))
- output 10: float32 [768, 3072], P(('ep', 'fsdp'))
- output 11: float32 [768, 3072], P(('ep', 'fsdp'))
- output 12: float32 [3072, 768], P(None, ('ep', 'fsdp'))
- output 13: float32 [8, 768, 3072], P('ep', 'fsdp')
- output 14: float32 [8, 768, 3072], P('ep', 'fsdp')
- output 15: float32 [8, 3072, 768], P('ep', 'fsdp')
All inputs are finite; a program needn't handle non-finite values.
Results may differ from the reference program's by a relative error of at most 0.02.
Values are sent between devices in bfloat16 or wider.
A program may use at most 1 GiB of HBM per device.

```python
import numpy as np
import jax
import jax.numpy as jnp
from jax import lax

DEVICES = 32
BATCH_DEV = 1
SEQ = 512
D = 768
HEADS = 12
KV_HEADS = 12
HEAD = 64
EXPERTS = 8
FF = 3072
FF_SH = 3072

BATCH_ALL = DEVICES * BATCH_DEV
TOKENS_DEV = BATCH_DEV * SEQ
CAPACITY = 2 * TOKENS_DEV // EXPERTS
Q_PER_KV = HEADS // KV_HEADS
Q_LEN = min(SEQ, 256)
EPS_NORM = 1e-5
EPS_QK = 1e-6
ROPE_BASE = 500000.0


def draw_expert_ids(root_key):
    hot_key, dev_key = jax.random.split(root_key)
    expert_order = jax.random.permutation(hot_key, EXPERTS)
    quarter = EXPERTS // 4
    per_expert = TOKENS_DEV // EXPERTS
    counts = np.array([2 * per_expert] * quarter + [per_expert] * quarter + [per_expert // 2] * (2 * quarter))
    base_ids = jnp.repeat(expert_order, counts, total_repeat_length=TOKENS_DEV)
    dev_keys = jax.random.split(dev_key, DEVICES)
    shuffled = jax.vmap(jax.random.permutation, in_axes=(0, None))(dev_keys, base_ids)
    return shuffled.reshape(BATCH_ALL, SEQ).astype(jnp.int32)


def setup_inputs(seed: int = 0) -> dict:
    sub_keys = jax.random.split(jax.random.key(seed), 16)

    def normal(draw_key, arr_shape, std_scale):
        return jax.random.normal(draw_key, arr_shape, jnp.float32) * std_scale

    x_in = normal(sub_keys[0], (BATCH_ALL, SEQ, D), 1.0).astype(jnp.bfloat16)
    grad_y = normal(sub_keys[1], (BATCH_ALL, SEQ, D), 1.0).astype(jnp.bfloat16)
    w_q = normal(sub_keys[2], (D, HEADS, HEAD), D ** -0.5).astype(jnp.bfloat16)
    w_k = normal(sub_keys[3], (D, KV_HEADS, HEAD), D ** -0.5).astype(jnp.bfloat16)
    w_v = normal(sub_keys[4], (D, KV_HEADS, HEAD), D ** -0.5).astype(jnp.bfloat16)
    w_o = normal(sub_keys[5], (HEADS, HEAD, D), 2.0 * (HEADS * HEAD) ** -0.5).astype(jnp.bfloat16)
    gamma_attn = (1.0 + 0.3 * normal(sub_keys[6], (D,), 1.0)).astype(jnp.bfloat16)
    gamma_mlp = (1.0 + 0.3 * normal(sub_keys[7], (D,), 1.0)).astype(jnp.bfloat16)
    w_router = normal(sub_keys[8], (D, EXPERTS), 0.6 * D ** -0.5)
    w1_shared = normal(sub_keys[9], (D, FF_SH), D ** -0.5).astype(jnp.bfloat16)
    w3_shared = normal(sub_keys[10], (D, FF_SH), D ** -0.5).astype(jnp.bfloat16)
    w2_shared = normal(sub_keys[11], (FF_SH, D), FF_SH ** -0.5).astype(jnp.bfloat16)
    w1_expert = normal(sub_keys[12], (EXPERTS, D, FF), 2.0 * D ** -0.5).astype(jnp.bfloat16)
    w3_expert = normal(sub_keys[13], (EXPERTS, D, FF), 2.0 * D ** -0.5).astype(jnp.bfloat16)
    w2_expert = normal(sub_keys[14], (EXPERTS, FF, D), FF ** -0.5).astype(jnp.bfloat16)
    expert_ids = draw_expert_ids(sub_keys[15])
    return {'x_in': x_in, 'grad_y': grad_y, 'w_q': w_q, 'w_k': w_k, 'w_v': w_v, 'w_o': w_o, 'gamma_attn': gamma_attn, 'gamma_mlp': gamma_mlp, 'w_router': w_router, 'w1_shared': w1_shared, 'w3_shared': w3_shared, 'w2_shared': w2_shared, 'w1_expert': w1_expert, 'w3_expert': w3_expert, 'w2_expert': w2_expert, 'expert_ids': expert_ids}


def rms_norm(tokens, gamma_vec):
    tok_f32 = tokens.astype(jnp.float32)
    inv_rms = lax.rsqrt(jnp.mean(tok_f32 * tok_f32, axis=-1, keepdims=True) + EPS_NORM)
    return (tok_f32 * inv_rms * gamma_vec.astype(jnp.float32)).astype(jnp.bfloat16)


def swiglu_act(up_gate, up_lin):
    return (jax.nn.silu(up_gate) * up_lin).astype(jnp.bfloat16)


def rope_tables():
    half_dim = HEAD // 2
    inv_freq = ROPE_BASE ** (-(jnp.arange(half_dim, dtype=jnp.float32) * 2.0 / HEAD))
    angles = jnp.arange(SEQ, dtype=jnp.float32)[:, None] * inv_freq[None, :]
    return jnp.cos(angles), jnp.sin(angles)


def rope_norm(heads_in, cos_tab, sin_tab):
    half_dim = heads_in.shape[-1] // 2
    head_vals = heads_in.astype(jnp.float32)
    first_half = head_vals[..., :half_dim]
    second_half = head_vals[..., half_dim:]
    cos_b = cos_tab[:, None, :]
    sin_b = sin_tab[:, None, :]
    rotated = jnp.concatenate([first_half * cos_b - second_half * sin_b, second_half * cos_b + first_half * sin_b], axis=-1)
    rotated = rotated * lax.rsqrt(jnp.mean(rotated * rotated, axis=-1, keepdims=True) + EPS_QK)
    return rotated.astype(jnp.bfloat16)


def seq_attention(seq_args):
    q_seq, k_seq, v_seq = seq_args
    cos_tab, sin_tab = rope_tables()
    q_rot = rope_norm(q_seq, cos_tab, sin_tab).reshape(SEQ // Q_LEN, Q_LEN, KV_HEADS, Q_PER_KV, HEAD)
    k_rot = rope_norm(k_seq, cos_tab, sin_tab).astype(jnp.float32)
    v_f32 = v_seq.astype(jnp.float32)
    key_pos = jnp.arange(SEQ)

    def one_block(blk_args):
        q_blk, blk_start = blk_args
        scores = jnp.einsum('qkgd,skd->kgqs', q_blk.astype(jnp.float32), k_rot) * HEAD ** -0.5
        causal = (blk_start + jnp.arange(Q_LEN))[:, None] >= key_pos[None, :]
        attn_probs = jax.nn.softmax(jnp.where(causal, scores, -1e30), axis=-1).astype(jnp.bfloat16)
        return jnp.einsum('kgqs,skd->qkgd', attn_probs.astype(jnp.float32), v_f32).astype(jnp.bfloat16)

    blocks_out = lax.map(jax.checkpoint(one_block), (q_rot, jnp.arange(SEQ // Q_LEN) * Q_LEN))
    return blocks_out.reshape(SEQ, HEADS, HEAD)


def layer_forward(x_in, w_q, w_k, w_v, w_o, gamma_attn, gamma_mlp, w_router, w1_shared, w3_shared, w2_shared, w1_expert, w3_expert, w2_expert, expert_ids):
    n_tok = BATCH_ALL * SEQ
    tokens = x_in.reshape(n_tok, D)
    normed1 = rms_norm(tokens, gamma_attn)
    normed1_f = normed1.astype(jnp.float32)
    q_proj = jnp.einsum('td,dhk->thk', normed1_f, w_q.astype(jnp.float32)).astype(jnp.bfloat16)
    k_proj = jnp.einsum('td,dhk->thk', normed1_f, w_k.astype(jnp.float32)).astype(jnp.bfloat16)
    v_proj = jnp.einsum('td,dhk->thk', normed1_f, w_v.astype(jnp.float32)).astype(jnp.bfloat16)
    attn_heads = lax.map(jax.checkpoint(seq_attention), (q_proj.reshape(BATCH_ALL, SEQ, HEADS, HEAD), k_proj.reshape(BATCH_ALL, SEQ, KV_HEADS, HEAD), v_proj.reshape(BATCH_ALL, SEQ, KV_HEADS, HEAD)))
    attn_out = jnp.einsum('thk,hkd->td', attn_heads.reshape(n_tok, HEADS, HEAD).astype(jnp.float32), w_o.astype(jnp.float32))
    hidden = (tokens.astype(jnp.float32) + attn_out).astype(jnp.bfloat16)
    normed2 = rms_norm(hidden, gamma_mlp)
    normed2_f = normed2.astype(jnp.float32)
    logits = jnp.dot(normed2_f, w_router)
    flat_ids = expert_ids.reshape(n_tok)
    gate_val = jax.nn.sigmoid(jnp.take_along_axis(logits, flat_ids[:, None], axis=1)[:, 0])
    routed_in = (gate_val[:, None] * normed2_f).astype(jnp.bfloat16)
    w1_f = w1_expert.astype(jnp.float32)
    w3_f = w3_expert.astype(jnp.float32)
    w2_f = w2_expert.astype(jnp.float32)

    def expert_block(blk_args):
        blk_in, blk_ids = blk_args
        onehot = blk_ids[:, None] == jnp.arange(EXPERTS)[None, :]
        running = jnp.cumsum(onehot.astype(jnp.int32), axis=0)
        dest_row = blk_ids * CAPACITY + jnp.sum(jnp.where(onehot, running, 0), axis=1) - 1
        buffer = jnp.zeros((EXPERTS * CAPACITY, D), jnp.bfloat16).at[dest_row].set(blk_in)
        buffer = buffer.reshape(EXPERTS, CAPACITY, D).astype(jnp.float32)
        up_gate = jnp.einsum('ecd,edf->ecf', buffer, w1_f)
        up_lin = jnp.einsum('ecd,edf->ecf', buffer, w3_f)
        act_rows = swiglu_act(up_gate, up_lin)
        down_rows = jnp.einsum('ecf,efd->ecd', act_rows.astype(jnp.float32), w2_f).astype(jnp.bfloat16)
        return down_rows.reshape(EXPERTS * CAPACITY, D)[dest_row]

    routed = lax.map(jax.checkpoint(expert_block), (routed_in.reshape(DEVICES, TOKENS_DEV, D), expert_ids.reshape(DEVICES, TOKENS_DEV))).reshape(n_tok, D)
    sh_gate = jnp.dot(normed2, w1_shared, preferred_element_type=jnp.float32)
    sh_lin = jnp.dot(normed2, w3_shared, preferred_element_type=jnp.float32)
    shared_out = jnp.dot(swiglu_act(sh_gate, sh_lin), w2_shared, preferred_element_type=jnp.float32)
    layer_out = (hidden.astype(jnp.float32) + routed.astype(jnp.float32) + shared_out).astype(jnp.bfloat16)
    return layer_out.reshape(BATCH_ALL, SEQ, D)


def reference(x_in, grad_y, w_q, w_k, w_v, w_o, gamma_attn, gamma_mlp, w_router, w1_shared, w3_shared, w2_shared, w1_expert, w3_expert, w2_expert, expert_ids):
    def forward(*params):
        return layer_forward(*params, expert_ids)

    layer_out, pullback = jax.vjp(forward, x_in, w_q, w_k, w_v, w_o, gamma_attn, gamma_mlp, w_router, w1_shared, w3_shared, w2_shared, w1_expert, w3_expert, w2_expert)
    grads = pullback(grad_y)
    return (layer_out, grads[0], grads[1].astype(jnp.float32), grads[2].astype(jnp.float32), grads[3].astype(jnp.float32), grads[4].astype(jnp.float32), grads[5].astype(jnp.float32), grads[6].astype(jnp.float32), grads[7].astype(jnp.float32), grads[8].astype(jnp.float32), grads[9].astype(jnp.float32), grads[10].astype(jnp.float32), grads[11].astype(jnp.float32), grads[12].astype(jnp.float32), grads[13].astype(jnp.float32))
```

```python
import jax
import jax.numpy as jnp
import numpy as np
from jax import lax
from jax.experimental import pallas as pl
from jax.experimental.pallas import tpu as pltpu
from jax.sharding import Mesh, PartitionSpec as P

EPS_NORM = 1e-5
EPS_QK = 1e-6
ROPE_BASE = 500000.0
QUERY_BLOCK = 256
AXES = ('z', 'y', 'x', 'c')
SWAP = ((0, 1), (1, 0))
F32 = jnp.float32
BF16 = jnp.bfloat16


def rms_norm(tokens, gamma_vec):
    tok_f32 = tokens.astype(F32)
    inv_rms = lax.rsqrt(jnp.mean(tok_f32 * tok_f32, axis=-1, keepdims=True) + EPS_NORM)
    return (tok_f32 * inv_rms * gamma_vec.astype(F32)).astype(BF16)


def swiglu_act(up_gate, up_lin):
    return (jax.nn.silu(up_gate) * up_lin).astype(BF16)


def rope_tables(seq_len, head_dim):
    half_dim = head_dim // 2
    inv_freq = ROPE_BASE ** (-(jnp.arange(half_dim, dtype=F32) * 2.0 / head_dim))
    angles = jnp.arange(seq_len, dtype=F32)[:, None] * inv_freq[None, :]
    return jnp.cos(angles), jnp.sin(angles)


def rope_norm(heads_in, cos_tab, sin_tab):
    half_dim = heads_in.shape[-1] // 2
    head_vals = heads_in.astype(F32)
    first_half = head_vals[..., :half_dim]
    second_half = head_vals[..., half_dim:]
    cos_b = cos_tab[:, None, :]
    sin_b = sin_tab[:, None, :]
    rotated = jnp.concatenate([first_half * cos_b - second_half * sin_b, second_half * cos_b + first_half * sin_b], axis=-1)
    rotated = rotated * lax.rsqrt(jnp.mean(rotated * rotated, axis=-1, keepdims=True) + EPS_QK)
    return rotated.astype(BF16)


def attention(q_proj, k_proj, v_proj):
    n_batch, seq_len, n_heads, head_dim = q_proj.shape
    kv_heads = k_proj.shape[2]
    q_per_kv = n_heads // kv_heads
    cos_tab, sin_tab = rope_tables(seq_len, head_dim)
    q_len = min(seq_len, QUERY_BLOCK)
    n_blocks = seq_len // q_len
    q_rot = rope_norm(q_proj, cos_tab, sin_tab).reshape(n_batch, n_blocks, q_len, kv_heads, q_per_kv, head_dim)
    q_blocks = jnp.moveaxis(q_rot, 1, 0)
    k_rot = rope_norm(k_proj, cos_tab, sin_tab)
    key_pos = jnp.arange(seq_len)

    def one_block(blk_args):
        q_blk, blk_start = blk_args
        scores = jnp.einsum('bqkgd,bskd->bkgqs', q_blk, k_rot, preferred_element_type=F32) * head_dim ** -0.5
        causal = (blk_start + jnp.arange(q_len))[:, None] >= key_pos[None, :]
        attn_probs = jax.nn.softmax(jnp.where(causal, scores, -1e30), axis=-1).astype(BF16)
        return jnp.einsum('bkgqs,bskd->bqkgd', attn_probs, v_proj, preferred_element_type=F32).astype(BF16)

    blocks_out = lax.map(jax.checkpoint(one_block), (q_blocks, jnp.arange(n_blocks) * q_len))
    return jnp.moveaxis(blocks_out, 0, 1).reshape(n_batch, seq_len, n_heads, head_dim)


def route_slots(flat_ids, n_experts, capacity):
    onehot = flat_ids[:, None] == jnp.arange(n_experts)[None, :]
    running = jnp.cumsum(onehot.astype(jnp.int32), axis=0)
    slot_idx = jnp.sum(jnp.where(onehot, running, 0), axis=1) - 1
    return onehot, flat_ids * capacity + slot_idx


def hop(block, axis):
    return lax.ppermute(block, axis, SWAP)


def z_hop(block, step):
    return lax.ppermute(block, 'z', [(z_idx, z_idx ^ step) for z_idx in range(4)])


def pick(array, idx, axis):
    return lax.dynamic_index_in_dim(array, idx, axis, keepdims=False)


def in_core_order(mine, other, axis):
    first = lax.axis_index('c') == 0
    return jnp.concatenate([jnp.where(first, mine, other), jnp.where(first, other, mine)], axis=axis)


def core_halves(array, axis):
    low, high = jnp.split(array, 2, axis=axis)
    first = lax.axis_index('c') == 0
    return jnp.where(first, low, high), jnp.where(first, high, low)


def place_kernel(sub, where_ref, own_ref, x_ref, y_ref, low_ref, high_ref, out_ref):
    rel, part = pl.program_id(0), pl.program_id(1)
    for rel_idx, src_ref in ((0, own_ref), (1, x_ref), (2, y_ref)):
        @pl.when(rel == rel_idx)
        def _(src_ref=src_ref):
            out_ref[...] = src_ref[...].reshape(out_ref.shape)

    @pl.when(jnp.logical_and(rel == 3, part < sub // 2))
    def _():
        out_ref[...] = low_ref[...].reshape(out_ref.shape)

    @pl.when(jnp.logical_and(rel == 3, part >= sub // 2))
    def _():
        out_ref[...] = high_ref[...].reshape(out_ref.shape)


def place_blocks(where, pieces, part_major):
    block = pieces[0]
    sub, rows, cols = block.shape
    half = sub // 2

    def src_map(rel_idx, first, count):
        def index(rel, part, where_ref):
            here = jnp.clip(part - first, 0, count - 1)
            return jnp.where(rel == rel_idx, here, jnp.where(rel < rel_idx, 0, count - 1)), 0, 0
        return index

    def out_map(rel, part, where_ref):
        block_idx, part_idx = rel ^ where_ref[0], part ^ where_ref[1]
        return (part_idx, block_idx, 0, 0) if part_major else (block_idx, part_idx, 0, 0)

    out_shape = (sub, 4, rows, cols) if part_major else (4, sub, rows, cols)
    specs = [pl.BlockSpec((1, rows, cols), src_map(rel_idx, first, count)) for rel_idx, first, count in ((0, 0, sub), (1, 0, sub), (2, 0, sub), (3, 0, half), (3, half, half))]
    return pl.pallas_call(
        lambda *refs: place_kernel(sub, *refs),
        grid_spec=pltpu.PrefetchScalarGridSpec(num_scalar_prefetch=1, grid=(4, sub), in_specs=specs, out_specs=pl.BlockSpec((1, 1, rows, cols), out_map)),
        out_shape=jax.ShapeDtypeStruct(out_shape, block.dtype),
        cost_estimate=pl.CostEstimate(flops=4 * sub * rows * cols, bytes_accessed=16 * sub * rows * cols, transcendentals=0),
    )(where, *pieces)


def plane_first(block):
    return block, hop(block, 'x'), hop(block, 'y')


def plane_last(first, z_rel, part_major):
    block, from_x, from_y = first
    half = block.shape[0] // 2
    low, high = hop(from_y[:half], 'x'), hop(from_x[half:], 'y')
    where = jnp.stack([2 * lax.axis_index('y') + lax.axis_index('x'), lax.axis_index('z') if z_rel else jnp.int32(0)]).astype(jnp.int32)
    return place_blocks(where, (block, from_x, from_y, low, high), part_major)


def after(value, *anchors):
    return lax.optimization_barrier((value,) + anchors)[0]


def z_stack(block):
    own, other = core_halves(block, 1)
    chip = in_core_order(own, hop(other, 'c'), 0)
    return jnp.stack([chip] + [z_hop(chip, step) for step in (1, 2, 3)])


def expert_chips(w1_expert, w3_expert, w2_expert):
    c_me = lax.axis_index('c')
    up = jnp.stack([w1_expert, w3_expert])
    up_chip = in_core_order(pick(up, c_me, 1), hop(pick(up, 1 - c_me, 1), 'c'), 1)
    down_chip = in_core_order(pick(w2_expert, c_me, 0), hop(pick(w2_expert, 1 - c_me, 0), 'c'), 0)
    return up_chip, down_chip.reshape(2, -1, down_chip.shape[1])


def dot32(lhs, rhs):
    return jnp.dot(lhs, rhs, preferred_element_type=F32)


class PlaneSum:
    anchor = None

    def hold(self, value):
        return value if self.anchor is None else after(value, self.anchor)

    def __init__(self, lhs_t, rhs, x_first):
        z_rows, rows = lhs_t.shape[:2]
        self.blocks = lhs_t.reshape(z_rows, 2, 2, rows // 4, lhs_t.shape[2])
        self.rhs = rhs
        y_me, x_me = lax.axis_index('y'), lax.axis_index('x')
        self.me_1, self.me_2, self.axis = (x_me, y_me, 2) if x_first else (y_me, x_me, 1)
        self.names = ('x', 'y') if x_first else ('y', 'x')
        self.send = self.times(pick(self.blocks, 1 - self.me_1, self.axis))

    def times(self, block):
        flat = block.reshape(-1, block.shape[-1])
        return dot32(flat, self.rhs).reshape(block.shape[:-1] + (self.rhs.shape[1],))

    def second(self):
        self.near = pick(self.blocks, self.me_1, self.axis)
        self.got = self.hold(hop(self.send, self.names[0]))
        self.send_2 = self.times(pick(self.near, 1 - self.me_2, 1)) + pick(self.got, 1 - self.me_2, 1)

    def result(self):
        got_2 = self.hold(hop(self.send_2, self.names[1]))
        return self.times(pick(self.near, self.me_2, 1)) + pick(self.got, self.me_2, 1) + got_2


def z_sum(plane):
    z_me = lax.axis_index('z')
    summed = pick(plane, z_me, 0)
    for step in (1, 2, 3):
        summed = summed + z_hop(pick(plane, z_me ^ step, 0), step)
    return summed


class ZFirstSum:
    def __init__(self, lhs_t, rhs):
        z_me = lax.axis_index('z')
        self.blocks, self.rhs, self.z_me = lhs_t, rhs, z_me
        self.sends = [dot32(pick(lhs_t, z_me ^ step, 0), rhs) for step in (1, 2, 3)]

    def second(self):
        self.total = dot32(pick(self.blocks, self.z_me, 0), self.rhs)
        for step, send in zip((1, 2, 3), self.sends):
            self.total = self.total + z_hop(send, step)

    def result(self):
        total = self.total.reshape(2, 2, -1, self.total.shape[1])
        for name, axis in (('x', 1), ('y', 0)):
            me = lax.axis_index(name)
            total = pick(total, me, axis) + hop(pick(total, 1 - me, axis), name)
        return total


def swap_rows(summed):
    halves = summed.reshape(2, summed.shape[0] // 2, summed.shape[1])
    c_me = lax.axis_index('c')
    return pick(halves, c_me, 0), hop(pick(halves, 1 - c_me, 0), 'c')


def plane_sum_values(total):
    y_me, x_me = lax.axis_index('y'), lax.axis_index('x')
    first, second = total[:2], total[2:]
    from_x = hop(pick(first, 1 - x_me, 2), 'x')
    from_y = hop(pick(second, 1 - y_me, 1), 'y')
    keep_x, keep_y = pick(first, x_me, 2), pick(second, y_me, 1)
    from_xy = hop(pick(keep_x, 1 - y_me, 1) + pick(from_x, 1 - y_me, 1), 'y')
    from_yx = hop(pick(keep_y, 1 - x_me, 1) + pick(from_y, 1 - x_me, 1), 'x')
    return jnp.concatenate([pick(keep_x, y_me, 1) + pick(from_x, y_me, 1) + from_xy, pick(keep_y, x_me, 1) + pick(from_y, x_me, 1) + from_yx], axis=0)


def swap_experts(summed):
    c_me = lax.axis_index('c')
    halves = summed.reshape(summed.shape[:-2] + (2, summed.shape[-2] // 2, summed.shape[-1]))
    axis = halves.ndim - 3
    mine, other = pick(halves, c_me, axis), hop(pick(halves, 1 - c_me, axis), 'c')
    return in_core_order(mine[None], other[None], 0)


def gather_small(block):
    for name in ('c', 'x', 'y'):
        other = hop(block, name)
        low = lax.axis_index(name) == 0
        block = jnp.stack([jnp.where(low, block, other), jnp.where(low, other, block)])
    z_me = lax.axis_index('z')
    parts = [block] + [z_hop(block, step) for step in (1, 2, 3)]
    return jnp.stack([lax.select_n(z_me ^ z_idx, *parts) for z_idx in range(4)])


def scatter_small(grad):
    sums = grad.reshape(4, 2, 2, 2, 24, -1)
    for axis, name in ((1, 'y'), (1, 'x'), (1, 'c')):
        me = lax.axis_index(name)
        sums = pick(sums, me, axis) + hop(pick(sums, 1 - me, axis), name)
    z_me = lax.axis_index('z')
    total = pick(sums, z_me, 0)
    for step in (1, 2, 3):
        total = total + z_hop(pick(sums, z_me ^ step, 0), step)
    return total


def device_step(x_in, grad_y, w_q, w_k, w_v, w_o, gamma_attn, gamma_mlp, w_router, w1_shared, w3_shared, w2_shared, w1_expert, w3_expert, w2_expert, expert_ids):
    n_batch, seq_len, model_dim = x_in.shape
    n_tok = n_batch * seq_len
    n_heads, head_dim = w_q.shape[1], w_q.shape[2]
    att_dim, att_half = n_heads * head_dim, n_heads * head_dim // 2
    n_experts = w_router.shape[1]
    ff_half = w1_shared.shape[1] // 2
    capacity = 2 * n_tok // n_experts
    n_slots = n_experts * capacity

    att_parts = (w_q.reshape(-1, att_dim), w_k.reshape(-1, att_dim), w_v.reshape(-1, att_dim), w_o.reshape(att_dim, -1).T)
    att_block = jnp.concatenate([part[:, :att_half] for part in att_parts] + [part[:, att_half:] for part in att_parts], axis=1)
    small = jnp.concatenate([gamma_attn.astype(F32)[:, None], gamma_mlp.astype(F32)[:, None], w_router, jnp.zeros((w_router.shape[0], 6), F32)], axis=1)
    small_all = gather_small(small).reshape(model_dim, 16)
    ga_all, gm_all, wr_all = small_all[:, 0], small_all[:, 1], small_all[:, 2:2 + n_experts]
    sh_parts = (w1_shared, w3_shared, w2_shared.T)
    sh_block = jnp.concatenate([part[:, :ff_half] for part in sh_parts] + [part[:, ff_half:] for part in sh_parts], axis=1)
    att_stack = z_stack(att_block)
    att_first = plane_first(att_stack)
    up_chip, down_chip = expert_chips(w1_expert, w3_expert, w2_expert)
    sh_block, up_chip, down_chip = (after(value, *att_first[1:]) for value in (sh_block, up_chip, down_chip))
    att_mine = plane_last(att_first, True, True).reshape(model_dim, -1)
    att_w = (att_mine, hop(att_mine, 'c'))
    sh_stack = z_stack(sh_block)
    down_first = plane_first(down_chip)
    up_chip = after(up_chip, sh_stack)
    sh_first = plane_first(sh_stack)
    w2e_all = plane_last(down_first, False, False).reshape(-1, model_dim)
    sh_w = plane_last(sh_first, True, True).reshape(model_dim, -1)
    up_all = plane_last(plane_first(up_chip), False, True)
    w1e_all, w3e_all = up_all[0].reshape(model_dim, -1), up_all[1].reshape(model_dim, -1)

    d_out = grad_y.reshape(n_tok, model_dim)
    onehot, dest_row = route_slots(expert_ids.reshape(n_tok), n_experts, capacity)
    d_send = jnp.zeros((n_slots, model_dim), BF16).at[dest_row].set(d_out)
    d_down = lax.all_to_all(d_send.reshape(n_experts, capacity, model_dim), ('z', 'c'), 0, 0, tiled=True).reshape(n_slots, model_dim)

    tokens = x_in.reshape(n_tok, model_dim)
    normed1, norm1_pull = jax.vjp(rms_norm, tokens, ga_all)
    qkv = [dot32(normed1, w_half[:, :3 * att_half]).astype(BF16) for w_half in att_w]
    q_proj, k_proj, v_proj = (jnp.concatenate([half[:, part * att_half:(part + 1) * att_half] for half in qkv], axis=1) for part in range(3))
    heads_shape = (n_batch, seq_len, n_heads, head_dim)
    attn_heads, attn_pull = jax.vjp(attention, q_proj.reshape(heads_shape), k_proj.reshape(heads_shape), v_proj.reshape(heads_shape))
    attn_flat = attn_heads.reshape(n_tok, att_dim)
    attn_parts = (attn_flat[:, :att_half], attn_flat[:, att_half:])
    wot = [w_half[:, 3 * att_half:] for w_half in att_w]
    attn_out = sum(jnp.einsum('tk,dk->td', part, w_half, preferred_element_type=F32) for part, w_half in zip(attn_parts, wot))
    hidden = (tokens.astype(F32) + attn_out).astype(BF16)
    normed2, norm2_pull = jax.vjp(rms_norm, hidden, gm_all)
    normed2_f = normed2.astype(F32)
    logits = jnp.dot(normed2, wr_all, preferred_element_type=F32, precision=lax.Precision.HIGHEST)
    gate_val = jax.nn.sigmoid(jnp.sum(jnp.where(onehot, logits, 0.0), axis=1))
    routed_in = (gate_val[:, None] * normed2_f).astype(BF16)
    send_rows = jnp.zeros((n_slots, model_dim), BF16).at[dest_row].set(routed_in)
    rows = lax.all_to_all(send_rows.reshape(n_experts, capacity, model_dim), ('z', 'c'), 0, 0, tiled=True).reshape(n_slots, model_dim)

    d_out_both = jnp.concatenate([d_out, hop(d_out, 'c')], axis=0)
    normed2_both = jnp.concatenate([normed2, hop(normed2, 'c')], axis=0)
    w_13, w_2t = sh_w[:, :2 * ff_half], sh_w[:, 2 * ff_half:]
    up = dot32(normed2_both, w_13)
    act, act_pull = jax.vjp(swiglu_act, up[:, :ff_half], up[:, ff_half:])
    shared_part = jnp.einsum('tf,df->td', act, w_2t, preferred_element_type=F32)
    d_gate, d_lin = act_pull(dot32(d_out_both, w_2t).astype(BF16))
    d_gate, d_lin = d_gate.astype(BF16), d_lin.astype(BF16)
    d_part = jnp.einsum('tf,df->td', d_gate, w_13[:, :ff_half], preferred_element_type=F32) + jnp.einsum('tf,df->td', d_lin, w_13[:, ff_half:], preferred_element_type=F32)
    normed2_t = normed2_both.T.reshape(4, -1, 2 * n_tok)
    d_out_t = d_out_both.T.reshape(4, -1, 2 * n_tok)
    s_w2s = ZFirstSum(d_out_t, act)
    s_w1s, s_w3s = PlaneSum(normed2_t, d_gate, True), PlaneSum(normed2_t, d_lin, False)
    rows = after(rows, s_w1s.send, s_w3s.send, *s_w2s.sends)
    shared_out = shared_part[:n_tok] + hop(shared_part[n_tok:], 'c')
    d_normed2 = d_part[:n_tok] + hop(d_part[n_tok:], 'c')

    up_gate, up_lin = dot32(rows, w1e_all), dot32(rows, w3e_all)
    act_routed, routed_pull = jax.vjp(swiglu_act, up_gate, up_lin)
    act_t = act_routed.T[None]
    d_half = model_dim // 2
    s_w2e = PlaneSum(act_t, d_down[:, :d_half], True), PlaneSum(act_t, d_down[:, d_half:], False)
    d_down = after(d_down, s_w2e[0].send, s_w2e[1].send)
    d_act_routed = jnp.einsum('td,fd->tf', d_down, w2e_all, preferred_element_type=F32).astype(BF16)
    d_up_gate, d_up_lin = routed_pull(d_act_routed)
    d_up_gate, d_up_lin = d_up_gate.astype(BF16), d_up_lin.astype(BF16)
    d_rows = (jnp.einsum('tf,df->td', d_up_gate, w1e_all, preferred_element_type=F32) + jnp.einsum('tf,df->td', d_up_lin, w3e_all, preferred_element_type=F32)).astype(BF16)
    d_up_gate, d_up_lin = after(d_up_gate, d_rows), after(d_up_lin, d_rows)
    d_back = lax.all_to_all(d_rows.reshape(n_experts, capacity, model_dim), ('z', 'c'), 0, 0, tiled=True).reshape(n_slots, model_dim)
    rows_t = rows.T[None]
    s_w1e, s_w3e = PlaneSum(rows_t, d_up_gate, True), PlaneSum(rows_t, d_up_lin, False)
    s_w1s.second()
    s_w3s.second()
    s_w2s.second()
    d_back = after(d_back, s_w1e.send, s_w3e.send, s_w1s.send_2, s_w3s.send_2)
    act_routed = after(act_routed, s_w1e.send, s_w3e.send)

    down_rows = dot32(act_routed, w2e_all).astype(BF16)
    back_rows = lax.all_to_all(down_rows.reshape(n_experts, capacity, model_dim), ('z', 'c'), 0, 0, tiled=True).reshape(n_slots, model_dim)
    routed = back_rows[dest_row]
    layer_out = (hidden.astype(F32) + routed.astype(F32) + shared_out).astype(BF16)

    d_routed_in = d_back[dest_row].astype(F32)
    d_normed2 = d_normed2 + gate_val[:, None] * d_routed_in
    d_gate_val = jnp.sum(d_routed_in * normed2_f, axis=1) * gate_val * (1.0 - gate_val)
    d_logits = jnp.where(onehot, d_gate_val[:, None], 0.0)
    g_wr = jnp.einsum('td,te->de', normed2_f, d_logits, precision=lax.Precision.HIGHEST)
    d_normed2 = d_normed2 + jnp.einsum('te,de->td', d_logits, wr_all, precision=lax.Precision.HIGHEST)
    d_hid_norm, g_gm = norm2_pull(d_normed2.astype(BF16))
    d_hidden = (d_out.astype(F32) + d_hid_norm.astype(F32)).astype(BF16)

    d_attn = jnp.concatenate([dot32(d_hidden, w_half).astype(BF16) for w_half in wot], axis=1)
    d_hidden_t, normed1_t = d_hidden.T, normed1.T
    g_wot = [dot32(d_hidden_t, part) for part in attn_parts]
    d_heads = [d_part.reshape(n_tok, att_dim) for d_part in attn_pull(d_attn.reshape(heads_shape))]
    d_qkv = [jnp.concatenate([d_part[:, half * att_half:(half + 1) * att_half] for d_part in d_heads], axis=1) for half in range(2)]
    for chain in (s_w1s, s_w3s, *s_w2e, s_w1e, s_w3e):
        chain.anchor = d_qkv[0]
    s_w2s.total = after(s_w2s.total, d_qkv[0])
    for chain in (*s_w2e, s_w1e, s_w3e):
        chain.second()
    g_qkv = [dot32(normed1_t, half) for half in d_qkv]
    g_att = jnp.concatenate([own + hop(other, 'c') for own, other in ((g_qkv[0], g_qkv[1]), (g_wot[0], g_wot[1]))], axis=1)
    g_att_mine, g_att_other = swap_rows(z_sum(plane_sum_values(g_att.reshape(4, 2, 2, 48, -1))))
    d_normed1 = sum(jnp.einsum('tk,dk->td', half, w_half[:, :3 * att_half], preferred_element_type=F32) for half, w_half in zip(d_qkv, att_w))
    d_tok_norm, g_ga = norm1_pull(d_normed1.astype(BF16))
    d_x = (d_hidden.astype(F32) + d_tok_norm.astype(F32)).astype(BF16).reshape(n_batch, seq_len, model_dim)

    g_small = scatter_small(jnp.concatenate([g_ga[:, None], g_gm[:, None], g_wr, jnp.zeros((model_dim, 6), F32)], axis=1))
    g_w2e = swap_experts(jnp.concatenate([chain.result()[0] for chain in s_w2e], axis=1))
    g_up = swap_experts(jnp.stack([s_w1e.result()[0], s_w3e.result()[0]]))
    g_sh = jnp.concatenate([z_sum(s_w1s.result()), z_sum(s_w3s.result()), s_w2s.result()], axis=1)
    g_sh_mine, g_sh_other = swap_rows(g_sh)
    g_att = in_core_order(g_att_mine.reshape(-1, 4, att_half), g_att_other.reshape(-1, 4, att_half), 2)
    g_q, g_k, g_v = (g_att[:, part].reshape(-1, n_heads, head_dim) for part in range(3))
    g_wo = g_att[:, 3].T.reshape(n_heads, head_dim, -1)
    g_sh = in_core_order(g_sh_mine.reshape(-1, 3, ff_half), g_sh_other.reshape(-1, 3, ff_half), 2)
    return (layer_out.reshape(n_batch, seq_len, model_dim), d_x, g_q, g_k, g_v, g_wo, g_small[:, 0], g_small[:, 1], g_small[:, 2:2 + n_experts], g_sh[:, 0], g_sh[:, 1], g_sh[:, 2].T, g_up[:, 0], g_up[:, 1], g_w2e)


def solution(mesh):
    fine_mesh = Mesh(np.asarray(mesh.devices).reshape(4, 2, 2, 2), AXES)
    tok_spec = P(AXES, None, None)
    mat_spec = P(AXES, None)
    vec_spec = P(AXES)
    wo_spec = P(None, None, AXES)
    w2s_spec = P(None, AXES)
    exp_spec = P('z', ('y', 'x', 'c'), None)
    in_specs = (tok_spec, tok_spec, tok_spec, tok_spec, tok_spec, wo_spec, vec_spec, vec_spec, mat_spec, mat_spec, mat_spec, w2s_spec, exp_spec, exp_spec, exp_spec, mat_spec)
    out_specs = (tok_spec, tok_spec, tok_spec, tok_spec, tok_spec, wo_spec, vec_spec, vec_spec, mat_spec, mat_spec, mat_spec, w2s_spec, exp_spec, exp_spec, exp_spec)
    return jax.shard_map(device_step, mesh=fine_mesh, in_specs=in_specs, out_specs=out_specs, check_vma=False)
```

```python
import jax
import jax.numpy as jnp
import numpy as np
from jax import lax
from jax.experimental import pallas as pl
from jax.experimental.pallas import tpu as pltpu
from jax.sharding import Mesh, PartitionSpec as P

EPS_NORM = 1e-5
EPS_QK = 1e-6
ROPE_BASE = 500000.0
QUERY_BLOCK = 256
VMEM_LIMIT = 60 * 1024 * 1024
AXES = ('z', 'y', 'x', 'c')
Z_STEPS = (1, 2, 3)
SWAP = ((0, 1), (1, 0))
F32 = jnp.float32
BF16 = jnp.bfloat16


def rms_norm(tokens, gamma_vec):
    tok_f32 = tokens.astype(F32)
    inv_rms = lax.rsqrt(jnp.mean(tok_f32 * tok_f32, axis=-1, keepdims=True) + EPS_NORM)
    return (tok_f32 * inv_rms * gamma_vec.astype(F32)).astype(BF16)


def rope_tables(seq_len, head_dim):
    half_dim = head_dim // 2
    inv_freq = ROPE_BASE ** (-(jnp.arange(half_dim, dtype=F32) * 2.0 / head_dim))
    angles = jnp.arange(seq_len, dtype=F32)[:, None] * inv_freq[None, :]
    cos_tab, sin_tab = jnp.cos(angles), jnp.sin(angles)
    return jnp.concatenate([cos_tab] * 4, axis=1), jnp.concatenate([-sin_tab, sin_tab] * 2, axis=1)


def lane_masks(rows):
    lane = lax.broadcasted_iota(jnp.int32, (rows, 128), 1)
    return lane % 64 < 32, lane < 64


def turn(vals, cos_tab, sin_tab, low_half):
    partner = jnp.where(low_half, pltpu.roll(vals, 96, 1), pltpu.roll(vals, 32, 1))
    return vals * cos_tab + partner * sin_tab


def head_mean(vals, head_a):
    sum_a = jnp.sum(jnp.where(head_a, vals, 0.0), axis=1, keepdims=True)
    sum_b = jnp.sum(jnp.where(head_a, 0.0, vals), axis=1, keepdims=True)
    return jnp.where(head_a, sum_a, sum_b) * (1.0 / 64)


def rope_norm(vals, cos_tab, sin_tab, low_half, head_a):
    rotated = turn(vals.astype(F32), cos_tab, sin_tab, low_half)
    inv = lax.rsqrt(head_mean(rotated * rotated, head_a) + EPS_QK)
    return rotated, inv, (rotated * inv).astype(BF16)


def rope_norm_back(d_out, rotated, inv, cos_tab, sin_tab, low_half, head_a):
    d_rot = inv * d_out - rotated * (inv * inv * inv * head_mean(d_out * rotated, head_a))
    return turn(d_rot, cos_tab, -sin_tab, low_half).astype(BF16)


def dot_nn(lhs, rhs):
    return jnp.einsum('ik,kj->ij', lhs, rhs, preferred_element_type=F32)


def dot_nt(lhs, rhs):
    return jnp.einsum('ik,jk->ij', lhs, rhs, preferred_element_type=F32)


def dot_tn(lhs, rhs):
    return jnp.einsum('ki,kj->ij', lhs, rhs, preferred_element_type=F32)


def softmax_block(q_rows, k_all, start, keys):
    scores = dot_nt(q_rows, k_all[:keys]) * 0.125
    row = start + lax.broadcasted_iota(jnp.int32, scores.shape, 0)
    col = lax.broadcasted_iota(jnp.int32, scores.shape, 1)
    scores = jnp.where(row >= col, scores, -1e30)
    weights = jnp.exp(scores - jnp.max(scores, axis=1, keepdims=True))
    return weights / jnp.sum(weights, axis=1, keepdims=True)


def attn_fwd_kernel(q_ref, k_ref, v_ref, cos_ref, sin_ref, o_ref):
    seq = q_ref.shape[0]
    low_half, head_a = lane_masks(seq)
    cos_tab, sin_tab = cos_ref[:], sin_ref[:]
    q_rot = rope_norm(q_ref[:], cos_tab, sin_tab, low_half, head_a)[-1]
    k_rot = rope_norm(k_ref[:], cos_tab, sin_tab, low_half, head_a)[-1]
    v_all = v_ref[:]
    zero = jnp.zeros_like(q_rot)
    q_heads = jnp.where(head_a, q_rot, zero), jnp.where(head_a, zero, q_rot)
    for start in range(0, seq, QUERY_BLOCK):
        keys = start + QUERY_BLOCK
        outs = [dot_nn(softmax_block(q_head[start:keys], k_rot, start, keys).astype(BF16), v_all[:keys]) for q_head in q_heads]
        o_ref[start:keys, :] = jnp.where(head_a[:QUERY_BLOCK], outs[0], outs[1]).astype(BF16)


def attn_bwd_kernel(q_ref, k_ref, v_ref, do_ref, cos_ref, sin_ref, dq_ref, dk_ref, dv_ref):
    seq = q_ref.shape[0]
    low_half, head_a = lane_masks(seq)
    cos_tab, sin_tab = cos_ref[:], sin_ref[:]
    q_raw, q_inv, q_rot = rope_norm(q_ref[:], cos_tab, sin_tab, low_half, head_a)
    k_raw, k_inv, k_rot = rope_norm(k_ref[:], cos_tab, sin_tab, low_half, head_a)
    v_all, d_o = v_ref[:], do_ref[:]
    zero = jnp.zeros_like(q_rot)
    grads = []
    for head in range(2):
        def only(vals, head=head):
            return jnp.where(head_a, vals, zero) if head == 0 else jnp.where(head_a, zero, vals)

        q_head, do_head = only(q_rot), only(d_o)
        dq_rows, dk_sum, dv_sum = [], None, None
        for start in range(0, seq, QUERY_BLOCK):
            keys = start + QUERY_BLOCK
            probs = softmax_block(q_head[start:keys], k_rot, start, keys)
            d_probs = dot_nt(do_head[start:keys], v_all[:keys])
            d_scores = probs * (d_probs - jnp.sum(probs * d_probs, axis=1, keepdims=True)) * 0.125
            d_scores = d_scores.astype(BF16)
            dq_rows.append(dot_nn(d_scores, k_rot[:keys]))
            dk_part = dot_tn(d_scores, q_head[start:keys])
            dv_part = dot_tn(probs.astype(BF16), do_head[start:keys])
            if keys < seq:
                pad = jnp.zeros((seq - keys, 128), F32)
                dk_part, dv_part = jnp.concatenate([dk_part, pad]), jnp.concatenate([dv_part, pad])
            dk_sum = dk_part if dk_sum is None else dk_sum + dk_part
            dv_sum = dv_part if dv_sum is None else dv_sum + dv_part
        grads.append((jnp.concatenate(dq_rows), dk_sum, dv_sum))
    d_q, d_k, d_v = (jnp.where(head_a, part_a, part_b) for part_a, part_b in zip(*grads))
    dq_ref[:] = rope_norm_back(d_q, q_raw, q_inv, cos_tab, sin_tab, low_half, head_a)
    dk_ref[:] = rope_norm_back(d_k, k_raw, k_inv, cos_tab, sin_tab, low_half, head_a)
    dv_ref[:] = d_v.astype(BF16)


def fixed(*shape):
    return pl.BlockSpec(shape, lambda *_: (0,) * len(shape))


def kernel_cost(flops, moved):
    return pl.CostEstimate(flops=flops, bytes_accessed=moved, transcendentals=0)


def attn_specs(seq, pairs):
    head_specs = [pl.BlockSpec((seq, 128), lambda pair, part=part: (0, part * pairs + pair)) for part in range(3)]
    one = pl.BlockSpec((seq, 128), lambda pair: (0, pair))
    table = fixed(seq, 128)
    return head_specs, one, table


def attn_fwd(qkv, cos_tab, sin_tab):
    seq, width = qkv.shape[0], qkv.shape[1] // 3
    head_specs, one, table = attn_specs(seq, width // 128)
    return pl.pallas_call(
        attn_fwd_kernel, grid=(width // 128,), in_specs=head_specs + [table, table], out_specs=one,
        out_shape=jax.ShapeDtypeStruct((seq, width), BF16),
        compiler_params=pltpu.CompilerParams(vmem_limit_bytes=VMEM_LIMIT),
        cost_estimate=kernel_cost(40 * seq * seq * width, seq * width),
    )(qkv, qkv, qkv, cos_tab, sin_tab)


def attn_bwd(qkv, d_o, cos_tab, sin_tab):
    seq, width = qkv.shape[0], qkv.shape[1] // 3
    head_specs, one, table = attn_specs(seq, width // 128)
    return pl.pallas_call(
        attn_bwd_kernel, grid=(width // 128,), in_specs=head_specs + [one, table, table], out_specs=[one] * 3,
        out_shape=[jax.ShapeDtypeStruct((seq, width), BF16)] * 3,
        compiler_params=pltpu.CompilerParams(vmem_limit_bytes=VMEM_LIMIT),
        cost_estimate=kernel_cost(80 * seq * seq * width, seq * width),
    )(qkv, qkv, qkv, d_o, cos_tab, sin_tab)


def route_slots(flat_ids, n_experts, capacity):
    onehot = flat_ids[:, None] == jnp.arange(n_experts)[None, :]
    running = jnp.cumsum(onehot.astype(jnp.int32), axis=0)
    slot_idx = jnp.sum(jnp.where(onehot, running, 0), axis=1) - 1
    return onehot, flat_ids * capacity + slot_idx


def hop(block, axis):
    return lax.ppermute(block, axis, SWAP)


def z_hop(block, step):
    return lax.ppermute(block, 'z', [(z_idx, z_idx ^ step) for z_idx in range(4)])


def pick(array, idx, axis):
    return lax.dynamic_index_in_dim(array, idx, axis, keepdims=False)


def in_core_order(mine, other, axis):
    first = lax.axis_index('c') == 0
    return jnp.concatenate([jnp.where(first, mine, other), jnp.where(first, other, mine)], axis=axis)


def plane_first(block):
    return block, hop(block, 'x'), hop(block, 'y')


def plane_pieces(first):
    block, from_x, from_y = first
    half = block.shape[0] // 2
    return block, from_x, from_y, hop(from_y[:half], 'x'), hop(from_x[half:], 'y')


def after(value, *anchors):
    return lax.optimization_barrier((value,) + anchors)[0]


def z_stack(parts):
    half = parts[0].shape[1] // 2
    c_me = lax.axis_index('c')

    def side(core):
        return jnp.concatenate([lax.dynamic_slice_in_dim(part, core * half, half, 1) for part in parts], axis=1)

    chip = in_core_order(side(c_me), hop(side(1 - c_me), 'c'), 0)
    return [chip] + [z_hop(chip, step) for step in Z_STEPS]


def weight_kernel(att_ref, small_ref, att_out, small_out, local_sems, send_sems, recv_sems):
    z_me, y_me, x_me, c_me = (lax.axis_index(name) for name in AXES)
    peers = [((z_me + step) % 4, y_me, x_me, c_me) for step in Z_STEPS]
    peer_x, peer_y, peer_c = (z_me, y_me, 1 - x_me, c_me), (z_me, 1 - y_me, x_me, c_me), (z_me, y_me, x_me, 1 - c_me)
    barrier = pltpu.get_barrier_semaphore()
    everyone = peers + [peer_x, peer_y, peer_c]
    for peer in everyone:
        pl.semaphore_signal(barrier, inc=1, device_id=peer, device_id_type=pl.DeviceIdType.MESH)
    pl.semaphore_wait(barrier, len(everyone))

    def slot(back, rel, core):
        y_at, x_at = (1 - y_me if rel >= 2 else y_me), (1 - x_me if rel % 2 else x_me)
        return (((z_me + 4 - back) % 4 * 2 + y_at) * 2 + x_at) * 2 + core

    pairs = ((att_ref, att_out), (small_ref, small_out))

    started = []

    def send(back, rel, peer, sem, own=False):
        at = slot(back, rel, c_me)
        for kind, (src, out) in enumerate(pairs):
            copy = pltpu.make_async_remote_copy(
                src_ref=src if own else out.at[at], dst_ref=out.at[at], send_sem=send_sems.at[kind, sem], recv_sem=recv_sems.at[kind, sem],
                device_id=peer, device_id_type=pl.DeviceIdType.MESH)
            copy.start()
            started.append(copy)

    def landed(back, rel, sem, core=c_me):
        for kind, (src, out) in enumerate(pairs):
            pltpu.make_async_copy(src, out.at[slot(back, rel, core)], recv_sems.at[kind, sem]).wait()

    z_sem, x_sem, y_sem, far_sem, c_sem = range(0, 20, 4)
    for step, peer in zip(Z_STEPS, peers):
        send(0, 0, peer, z_sem + step, own=True)
    for back in range(4):
        if back:
            landed(back, 0, z_sem + back)
        send(back, 0, peer_x, x_sem + back, own=not back)
        send(back, 0, peer_y, y_sem + back, own=not back)
        send(back, 0, peer_c, c_sem + 4 * back, own=not back)
    for back in range(4):
        landed(back, 1, x_sem + back)
        if back >= 2:
            send(back, 1, peer_y, far_sem + back)
        send(back, 1, peer_c, c_sem + 4 * back + 1)
        landed(back, 2, y_sem + back)
        if back < 2:
            send(back, 2, peer_x, far_sem + back)
        send(back, 2, peer_c, c_sem + 4 * back + 2)
    for back in range(4):
        landed(back, 3, far_sem + back)
        send(back, 3, peer_c, c_sem + 4 * back + 3)
    local = [pltpu.make_async_copy(src, out.at[slot(0, 0, c_me)], local_sems.at[kind]) for kind, (src, out) in enumerate(pairs)]
    for copy in local:
        copy.start()
    for back in range(4):
        for rel in range(4):
            landed(back, rel, c_sem + 4 * back + rel, 1 - c_me)
    for copy in local:
        copy.wait()
    for copy in started:
        copy.wait_send()


def gather_weights(att_block, small):
    any_spec = pl.BlockSpec(memory_space=pl.ANY)
    blocks = (att_block, small)
    return pl.pallas_call(
        weight_kernel, in_specs=[any_spec] * 2, out_specs=[any_spec] * 2,
        out_shape=[jax.ShapeDtypeStruct((32,) + block.shape, block.dtype) for block in blocks],
        scratch_shapes=[pltpu.SemaphoreType.DMA((2,)), pltpu.SemaphoreType.DMA((2, 32)), pltpu.SemaphoreType.DMA((2, 32))],
        compiler_params=pltpu.CompilerParams(collective_id=0, has_side_effects=True),
        cost_estimate=kernel_cost(att_block.size * 10 ** 5, att_block.size),
    )(*blocks)


def expert_chips(w1_expert, w3_expert, w2_expert):
    c_me = lax.axis_index('c')
    up = jnp.stack([w1_expert, w3_expert])
    up_chip = in_core_order(pick(up, c_me, 1), hop(pick(up, 1 - c_me, 1), 'c'), 1)
    down_chip = in_core_order(pick(w2_expert, c_me, 0), hop(pick(w2_expert, 1 - c_me, 0), 'c'), 0)
    return up_chip, down_chip.reshape(2, -1, down_chip.shape[1])


def dot32(lhs, rhs):
    return jnp.dot(lhs, rhs, preferred_element_type=F32)


def ffn_rows(rows_ref, dd_ref, w1_ref, w3_ref, w2_ref, w2_turned, wait_w2, act_ref, dg_ref, dl_ref, out_acc, back_acc):
    chunk = 512

    def step(idx, carry):
        at = pl.ds(pl.multiple_of(idx * chunk, chunk), chunk)
        gate, lin = dot_nn(rows_ref[at, :], w1_ref[:]), dot_nn(rows_ref[at, :], w3_ref[:])
        sig = jax.nn.sigmoid(gate)
        silu = gate * sig
        act = (silu * lin).astype(BF16)
        act_ref[at, :] = act
        if wait_w2 is not None:
            wait_w2(idx)
        w2 = w2_ref[:]
        d_act = (dot_nn(dd_ref[at, :], w2) if w2_turned else dot_nt(dd_ref[at, :], w2)).astype(BF16).astype(F32)
        d_lin = (d_act * silu).astype(BF16)
        d_gate = (d_act * lin * (sig + silu * (1.0 - sig))).astype(BF16)
        dg_ref[at, :] = d_gate
        dl_ref[at, :] = d_lin
        out_acc[at, :] += dot_nt(act, w2) if w2_turned else dot_nn(act, w2)
        back_acc[at, :] += dot_nt(d_gate, w1_ref[:]) + dot_nt(d_lin, w3_ref[:])
        return carry

    lax.fori_loop(0, rows_ref.shape[0] // chunk, step, 0)


def up_grads(lhs_s, dg_s, dl_s, g1_away, g1_near, g3_away, g3_near):
    for slot in range(2):
        for ref, rel, grad in ((g1_away, 2 * slot + 1, dg_s), (g1_near, 2 * slot, dg_s), (g3_away, slot + 2, dl_s), (g3_near, slot, dl_s)):
            ref[slot] = dot_nn(lhs_s[rel], grad[:])


def expert_kernel(half, info, rows_ref, dd_ref, rows_t_ref, dd_t_ref, *refs):
    up_refs, down_refs, refs = refs[:8], refs[8:13], refs[13:]
    if half == 1:
        acc_in, refs = refs[:2], refs[2:]
    out_ref, back_ref, g1_away, g1_near, g3_away, g3_near, g2_away, g2_near = refs[:8]
    w1, w3, w2, act_s, dg_s, dl_s, out_acc, back_acc, lhs_s, sems = refs[8:]
    step, me = pl.program_id(0), info[0]
    same_y = (me // 2) == half
    pieces = [(ref.at[0], ref.at[1]) for ref in down_refs[:3]] + [[ref.at[0] for ref in down_refs[3:]]]
    w2_halves = [w2.at[pl.ds(part * 384, 384)] for part in range(2)]
    for rel, srcs in enumerate(pieces):
        @pl.when(jnp.logical_and(same_y == (rel < 2), (step == 0) == (rel % 2 == 1)))
        def _(srcs=srcs):
            for part, src in enumerate(srcs):
                pltpu.make_async_copy(src, w2_halves[part], sems.at[part]).start()

    @pl.when(step == 0)
    def _():
        if half == 1:
            out_acc[:] = acc_in[0][:]
            back_acc[:] = acc_in[1][:]
        else:
            out_acc[:] = jnp.zeros_like(out_acc)
            back_acc[:] = jnp.zeros_like(back_acc)
        for rel in range(4):
            lhs_s[rel] = rows_t_ref[pl.ds(pl.multiple_of((me ^ rel) * 192, 64), 192), :]

    for rel in range(4):
        at = pl.ds(pl.multiple_of((me ^ rel) * 192, 64), 192)
        w1[at, :] = up_refs[rel][0]
        w3[at, :] = up_refs[4 + rel][0]

    def wait_w2(idx):
        @pl.when(idx == 0)
        def _():
            for part, src in enumerate(pieces[0]):
                pltpu.make_async_copy(src, w2_halves[part], sems.at[part]).wait()

    ffn_rows(rows_ref, dd_ref, w1, w3, w2, False, wait_w2, act_s, dg_s, dl_s, out_acc, back_acc)
    up_grads(lhs_s, dg_s, dl_s, g1_away, g1_near, g3_away, g3_near)

    for near in range(2):
        @pl.when(step == near)
        def _(g2_ref=(g2_away, g2_near)[near]):
            for part in range(2):
                at = slice(part * 384, part * 384 + 384)
                g2_ref[at, :] = dot_nn(dd_t_ref[at, :], act_s[:])

    @pl.when(step == 1)
    def _():
        out_ref[:] = out_acc[:].astype(out_ref.dtype)
        back_ref[:] = back_acc[:].astype(back_ref.dtype)


def expert_half(half, rows, dd, rows_t, dd_t, up, down, acc):
    tok, dim = rows.shape
    y_me, x_me = lax.axis_index('y'), lax.axis_index('x')
    info = jnp.stack([2 * y_me + x_me, 2 * half + 1 - x_me, 2 * half + x_me]).astype(jnp.int32)
    whole, turned = fixed(tok, dim), fixed(dim, tok)

    def up_spec(mat):
        return pl.BlockSpec((1, dim // 4, dim), lambda step, info_ref, mat=mat: (mat, 0, info_ref[1 + step]))

    own, from_x, from_y, low, high = up
    up_args = (own, from_x, from_y, low, own, from_x, from_y, high)
    up_specs = [up_spec(0)] * 4 + [up_spec(1)] * 3 + [up_spec(0)]
    any_spec = pl.BlockSpec(memory_space=pl.ANY)
    row_out = pl.BlockSpec((2, dim // 4, dim), lambda step, info_ref: (0, 0, info_ref[1 + step] - 2 * half))
    square = fixed(dim, dim)
    acc_type = F32 if half == 0 else BF16
    row_shape, square_shape = jax.ShapeDtypeStruct((2, dim // 4, 2 * dim), F32), jax.ShapeDtypeStruct((dim, dim), F32)
    return pl.pallas_call(
        lambda *refs: expert_kernel(half, *refs),
        grid_spec=pltpu.PrefetchScalarGridSpec(
            num_scalar_prefetch=1, grid=(2,),
            in_specs=[whole, whole, turned, turned] + up_specs + [any_spec] * 5 + [whole] * len(acc),
            out_specs=[whole, whole] + [row_out] * 4 + [square] * 2,
            scratch_shapes=[pltpu.VMEM((dim, dim), BF16)] * 3 + [pltpu.VMEM((tok, dim), BF16)] * 3 + [pltpu.VMEM((tok, dim), F32)] * 2 + [pltpu.VMEM((4, dim // 4, tok), BF16), pltpu.SemaphoreType.DMA((2,))]),
        out_shape=[jax.ShapeDtypeStruct((tok, dim), acc_type)] * 2 + [row_shape] * 4 + [square_shape] * 2,
        compiler_params=pltpu.CompilerParams(vmem_limit_bytes=VMEM_LIMIT),
        cost_estimate=kernel_cost(36 * tok * dim * dim, dim * dim),
    )(info, rows, dd, rows_t, dd_t, *up_args, *down, *acc)


def shared_kernel(info, rows_ref, dd_ref, rows_t_ref, dd_t_ref, *refs):
    pieces, refs = [refs[5 * mat:5 * mat + 5] for mat in range(3)], refs[15:]
    out_ref, back_ref, g1_away, g1_near, g3_away, g3_near = refs[:6]
    g2_refs = refs[6:10]
    w1, w3, w2, act_s, dg_s, dl_s, lhs_s, dd_s = refs[10:]
    step, me, z_me = pl.program_id(0), info[0], info[1]

    def spot(rel, turn_z):
        return pl.ds(pl.multiple_of(((z_me ^ turn_z) * 4 + (me ^ rel)) * 48, 16), 48)

    @pl.when(step == 0)
    def _():
        out_ref[:] = jnp.zeros_like(out_ref)
        back_ref[:] = jnp.zeros_like(back_ref)
        for rel in range(4):
            for turn_z in range(4):
                lhs_s[rel, turn_z * 48:(turn_z + 1) * 48, :] = rows_t_ref[spot(rel, turn_z), :]
                dd_s[turn_z, rel * 48:(rel + 1) * 48, :] = dd_t_ref[spot(rel, turn_z), :]

    for w_ref, (own, from_x, from_y, low, high) in zip((w1, w3, w2), pieces):
        for turn_z in range(4):
            for rel, src in ((0, own.at[turn_z]), (1, from_x.at[turn_z]), (2, from_y.at[turn_z]), (3, low.at[turn_z] if turn_z < 2 else high.at[turn_z - 2])):
                w_ref[spot(rel, turn_z), :] = src[:]

    ffn_rows(rows_ref, dd_ref, w1, w3, w2, True, None, act_s, dg_s, dl_s, out_ref, back_ref)
    up_grads(lhs_s, dg_s, dl_s, g1_away, g1_near, g3_away, g3_near)
    for turn_z in range(4):
        g2_refs[turn_z][:] = dot_nn(dd_s[turn_z], act_s[:])


def shared_ffn(rows, dd, rows_t, dd_t, pieces):
    tok, dim = rows.shape
    width = pieces[0].shape[2] // 3
    steps = width // dim
    info = jnp.stack([2 * lax.axis_index('y') + lax.axis_index('x'), lax.axis_index('z')]).astype(jnp.int32)
    whole, turned = fixed(tok, dim), fixed(dim, tok)
    piece_specs = [pl.BlockSpec((piece.shape[0], 48, dim), lambda step, info_ref, mat=mat: (0, 0, mat * steps + step)) for mat in range(3) for piece in pieces]
    row_out = pl.BlockSpec((2, dim // 4, dim), lambda step, info_ref: (0, 0, step))
    z_out = pl.BlockSpec((dim // 4, dim), lambda step, info_ref: (0, step))
    return pl.pallas_call(
        shared_kernel,
        grid_spec=pltpu.PrefetchScalarGridSpec(
            num_scalar_prefetch=1, grid=(steps,),
            in_specs=[whole, whole, turned, turned] + piece_specs,
            out_specs=[whole, whole] + [row_out] * 4 + [z_out] * 4,
            scratch_shapes=[pltpu.VMEM((dim, dim), BF16)] * 3 + [pltpu.VMEM((tok, dim), BF16)] * 3 + [pltpu.VMEM((4, dim // 4, tok), BF16)] * 2),
        out_shape=[jax.ShapeDtypeStruct((tok, dim), F32)] * 2 + [jax.ShapeDtypeStruct((2, dim // 4, width), F32)] * 4 + [jax.ShapeDtypeStruct((dim // 4, width), F32)] * 4,
        compiler_params=pltpu.CompilerParams(vmem_limit_bytes=VMEM_LIMIT),
        cost_estimate=kernel_cost(18 * tok * dim * width, dim * width),
    )(info, rows, dd, rows_t, dd_t, *(list(pieces) * 3))


def z_sum(plane):
    summed = plane[0]
    for step in (1, 2, 3):
        summed = summed + z_hop(plane[step], step)
    return summed


def swap_rows(summed):
    halves = summed.reshape(summed.shape[:-2] + (2, -1, summed.shape[-1]))
    axis, c_me = halves.ndim - 3, lax.axis_index('c')
    return pick(halves, c_me, axis), hop(pick(halves, 1 - c_me, axis), 'c')


def plane_sum_values(total):
    y_me, x_me = lax.axis_index('y'), lax.axis_index('x')
    ways = tuple(zip((total[:2], total[2:]), ((2, x_me, y_me, 'x', 'y'), (1, y_me, x_me, 'y', 'x'))))
    gives = [pick(part, 1 - me_1, axis_1) for part, (axis_1, me_1, *_) in ways]

    def rest():
        planes = []
        for give, (part, (axis_1, me_1, me_2, name_1, name_2)) in zip(gives, ways):
            got, keep = hop(give, name_1), pick(part, me_1, axis_1)
            got_2 = hop(pick(keep, 1 - me_2, 1) + pick(got, 1 - me_2, 1), name_2)
            planes.append(pick(keep, me_2, 1) + pick(got, me_2, 1) + got_2)
        return jnp.concatenate(planes, axis=0)

    return gives, rest


def swap_experts(summed):
    return in_core_order(*(part[None] for part in swap_rows(summed)), 0)


def scatter_small(grad):
    sums = grad.reshape(4, 2, 2, 2, 24, -1)
    for axis, name in ((1, 'y'), (1, 'x'), (1, 'c')):
        me = lax.axis_index(name)
        sums = pick(sums, me, axis) + hop(pick(sums, 1 - me, axis), name)
    z_me = lax.axis_index('z')
    total = pick(sums, z_me, 0)
    for step in (1, 2, 3):
        total = total + z_hop(pick(sums, z_me ^ step, 0), step)
    return total


def layer_step(x_in, grad_y, w_q, w_k, w_v, w_o, gamma_attn, gamma_mlp, w_router, w1_shared, w3_shared, w2_shared, w1_expert, w3_expert, w2_expert, expert_ids):
    n_batch, seq_len, model_dim = x_in.shape
    n_tok = n_batch * seq_len
    n_heads, head_dim = w_q.shape[1], w_q.shape[2]
    att_dim, att_half = n_heads * head_dim, n_heads * head_dim // 2
    n_experts = w_router.shape[1]
    ff_half = w1_shared.shape[1] // 2
    capacity = 2 * n_tok // n_experts
    n_slots = n_experts * capacity

    att_parts = (w_q.reshape(-1, att_dim), w_k.reshape(-1, att_dim), w_v.reshape(-1, att_dim), w_o.reshape(att_dim, -1).T)
    att_block = jnp.concatenate([part[:, :att_half] for part in att_parts] + [part[:, att_half:] for part in att_parts], axis=1)
    small = jnp.concatenate([gamma_attn.astype(F32)[:, None], gamma_mlp.astype(F32)[:, None], w_router], axis=1)
    small = jnp.pad(small, ((0, 0), (0, 128 - small.shape[1])))
    up_chip, down_chip = expert_chips(w1_expert, w3_expert, w2_expert)
    att_all, small_all = gather_weights(att_block, small)
    att_all, small_all = att_all.reshape(model_dim, -1), small_all.reshape(model_dim, -1)
    att_w = jnp.split(att_all, 2, axis=1)
    ga_all, gm_all, wr_all = small_all[:, 0], small_all[:, 1], small_all[:, 2:2 + n_experts]
    down_first = plane_first(down_chip)
    up_first = plane_first(up_chip)
    sh_parts = z_stack((w1_shared, w3_shared, w2_shared.T))

    d_out = grad_y.reshape(n_tok, model_dim)
    onehot, dest_row = route_slots(expert_ids.reshape(n_tok), n_experts, capacity)
    place = (dest_row[:, None] == jnp.arange(n_slots)[None, :]).astype(BF16)

    def exchange(values):
        return lax.all_to_all(values.reshape(n_experts, capacity, model_dim), ('z', 'c'), 0, 0, tiled=True).reshape(n_slots, model_dim)

    def dispatch(values):
        return exchange(jnp.einsum('ts,td->sd', place, values, preferred_element_type=F32).astype(BF16))

    d_out_both = jnp.concatenate([d_out, hop(d_out, 'c')], axis=0)
    d_out_t = d_out_both.T
    cos_tab, sin_tab = rope_tables(seq_len, head_dim)

    tokens = x_in.reshape(n_tok, model_dim)
    normed1, norm1_pull = jax.vjp(rms_norm, tokens, ga_all)
    qkv = [dot32(normed1, w_half[:, :3 * att_half]).astype(BF16) for w_half in att_w]
    attn_parts = [attn_fwd(half, cos_tab, sin_tab) for half in qkv]
    wot = [w_half[:, 3 * att_half:] for w_half in att_w]
    attn_out = sum(jnp.einsum('tk,dk->td', part, w_half, preferred_element_type=F32) for part, w_half in zip(attn_parts, wot))
    hidden = (tokens.astype(F32) + attn_out).astype(BF16)
    normed2, norm2_pull = jax.vjp(rms_norm, hidden, gm_all)
    normed2_f = normed2.astype(F32)
    logits = jnp.dot(normed2, wr_all, preferred_element_type=F32, precision=lax.Precision.HIGHEST)
    gate_val = jax.nn.sigmoid(jnp.sum(jnp.where(onehot, logits, 0.0), axis=1))
    routed_in = (gate_val[:, None] * normed2_f).astype(BF16)
    rows = dispatch(routed_in)
    d_down = dispatch(after(d_out, routed_in))
    d_down_t = d_down.T

    normed2_both = jnp.concatenate([normed2, hop(normed2, 'c')], axis=0)
    sh_first = plane_first(jnp.stack([after(part, attn_parts[1]) for part in sh_parts]))
    sh_pieces = plane_pieces([after(piece, routed_in) for piece in sh_first])
    down_pieces = plane_pieces([after(piece, routed_in) for piece in down_first])
    up_pieces = plane_pieces([after(piece, routed_in) for piece in up_first])
    shared_part, d_part, s1_away, s1_near, s3_away, s3_near, *s2 = shared_ffn(normed2_both, d_out_both, normed2_both.T, d_out_t, sh_pieces)
    shared_out = shared_part[:n_tok] + hop(shared_part[n_tok:], 'c')
    d_normed2 = d_part[:n_tok] + hop(d_part[n_tok:], 'c')

    rows_t = rows.T
    *acc, a1_away, a1_near, a3_away, a3_near, a2_away, a2_near = expert_half(0, rows, d_down, rows_t, d_down_t, up_pieces, down_pieces, ())
    down_rows, d_rows, b1_away, b1_near, b3_away, b3_near, b2_away, b2_near = expert_half(1, rows, d_down, rows_t, d_down_t, up_pieces, down_pieces, acc)
    d_back = exchange(d_rows)

    def first_sum(away, near, axis, gate):
        keep, give = near + after(hop(away, axis), *gate)
        return keep, hop(give, 'y' if axis == 'x' else 'x')

    s1, s3 = first_sum(s1_away, s1_near, 'x', [d_rows]), first_sum(s3_away, s3_near, 'y', [d_rows])
    a1, a3 = first_sum(a1_away, a1_near, 'x', [d_rows]), first_sum(a3_away, a3_near, 'y', [d_rows])
    routed = jnp.einsum('ts,sd->td', place, exchange(down_rows), preferred_element_type=F32)
    layer_out = (hidden.astype(F32) + routed + shared_out).astype(BF16)

    d_routed_in = jnp.einsum('ts,sd->td', place, d_back, preferred_element_type=F32)
    d_normed2 = d_normed2 + gate_val[:, None] * d_routed_in
    d_gate_val = jnp.sum(d_routed_in * normed2_f, axis=1) * gate_val * (1.0 - gate_val)
    d_logits = jnp.where(onehot, d_gate_val[:, None], 0.0)
    g_wr = jnp.einsum('td,te->de', normed2_f, d_logits, precision=lax.Precision.HIGHEST)
    d_normed2 = d_normed2 + jnp.einsum('te,de->td', d_logits, wr_all, precision=lax.Precision.HIGHEST)
    d_hid_norm, g_gm = norm2_pull(d_normed2.astype(BF16))
    d_hidden = (d_out.astype(F32) + d_hid_norm.astype(F32)).astype(BF16)

    d_hidden_t, normed1_t = d_hidden.T, normed1.T
    d_qkv = [jnp.concatenate(attn_bwd(half, dot32(d_hidden, w_half).astype(BF16), cos_tab, sin_tab), axis=1) for half, w_half in zip(qkv, wot)]
    c_me = lax.axis_index('c')
    core_0 = c_me == 0

    def core_pick(pair):
        first, second = pair
        return jnp.where(core_0, first, second), jnp.where(core_0, second, first)

    g_att = []
    for lhs_t, pair in ((normed1_t, d_qkv), (d_hidden_t, attn_parts)):
        mine, other = core_pick(pair)
        g_att.append(dot32(lhs_t, mine) + hop(dot32(lhs_t, other), 'c'))
    att_gives, att_rest = plane_sum_values(jnp.concatenate(g_att, axis=1).reshape(4, 2, 2, 48, -1))

    def later(value):
        return after(value, *att_gives)

    s2_total = s2[0]
    for step in Z_STEPS:
        s2_total = s2_total + later(z_hop(s2[step], step))
    b1, b3 = first_sum(b1_away, b1_near, 'x', att_gives), first_sum(b3_away, b3_near, 'y', att_gives)
    low_y = lax.axis_index('y') == 0
    g2_sums = a2_near + later(hop(a2_away, 'x')), b2_near + later(hop(b2_away, 'x'))
    g2_low, g2_high = g2_sums
    g2_keep, g2_give = jnp.where(low_y, g2_low, g2_high), jnp.where(low_y, g2_high, g2_low)

    def finish(pairs):
        return jnp.concatenate([mine + later(got) for mine, got in pairs], axis=1)

    g_w1, g_w3 = finish((a1, b1)), finish((a3, b3))
    g_w2 = (g2_keep + hop(g2_give, 'y')).T
    s2_keep, s2_give = jnp.split(s2_total.reshape(2, 2, 48, -1), 2, axis=1)
    s2_keep, s2_give = s2_keep + hop(s2_give, 'x')
    g_s2 = (s2_keep + hop(s2_give, 'y')).reshape(48, -1)
    g_sh = jnp.concatenate([z_sum(finish((pair,)).reshape(4, 48, -1)) for pair in (s1, s3)] + [g_s2], axis=1)
    g_sh_mine, g_sh_other = swap_rows(g_sh)
    g_w2e = swap_experts(g_w2)
    g_up = swap_experts(jnp.stack([g_w1, g_w3]))
    z_me = lax.axis_index('z')
    att_plane = att_rest()
    g_att_mine, g_att_other = swap_rows(z_sum([pick(att_plane, z_me ^ step, 0) for step in range(4)]))
    d_normed1 = sum(jnp.einsum('tk,dk->td', half, w_half[:, :3 * att_half], preferred_element_type=F32) for half, w_half in zip(d_qkv, att_w))
    d_tok_norm, g_ga = norm1_pull(d_normed1.astype(BF16))
    d_x = (d_hidden.astype(F32) + d_tok_norm.astype(F32)).astype(BF16).reshape(n_batch, seq_len, model_dim)

    g_small = scatter_small(later(jnp.concatenate([g_ga[:, None], g_gm[:, None], g_wr, jnp.zeros((model_dim, 6), F32)], axis=1)))
    g_att = in_core_order(g_att_mine.reshape(-1, 4, att_half), g_att_other.reshape(-1, 4, att_half), 2)
    g_q, g_k, g_v = (g_att[:, part].reshape(-1, n_heads, head_dim) for part in range(3))
    g_wo = g_att[:, 3].T.reshape(n_heads, head_dim, -1)
    g_sh = in_core_order(g_sh_mine.reshape(-1, 3, ff_half), g_sh_other.reshape(-1, 3, ff_half), 2)
    return (layer_out.reshape(n_batch, seq_len, model_dim), d_x, g_q, g_k, g_v, g_wo, g_small[:, 0], g_small[:, 1], g_small[:, 2:2 + n_experts], g_sh[:, 0], g_sh[:, 1], g_sh[:, 2].T, g_up[:, 0], g_up[:, 1], g_w2e)


def solution(mesh):
    fine_mesh = Mesh(np.asarray(mesh.devices).reshape(4, 2, 2, 2), AXES)
    row_spec, wo_spec, w2s_spec, exp_spec = P(AXES), P(None, None, AXES), P(None, AXES), P('z', AXES[1:])
    weight_specs = (row_spec,) * 3 + (wo_spec,) + (row_spec,) * 5 + (w2s_spec,) + (exp_spec,) * 3
    out_specs = (row_spec, row_spec) + weight_specs
    in_specs = out_specs + (row_spec,)
    return jax.shard_map(layer_step, mesh=fine_mesh, in_specs=in_specs, out_specs=out_specs, check_vma=False)
```

```python
import jax
import jax.numpy as jnp
import numpy as np
from jax import lax
from jax.experimental import pallas as pl
from jax.experimental.pallas import tpu as pltpu
from jax.sharding import Mesh, PartitionSpec as P

LANES = 128
ROWS = 48
QUAD = 4
EPS_NORM = 1e-5
EPS_QK = 1e-6
ROPE_BASE = 500000.0
QUERY_BLOCK = 256
VMEM_LIMIT = 60 * 1024 * 1024
AXES = ('z', 'y', 'x', 'c')
Z_STEPS = (1, 2, 3)
SWAP = ((0, 1), (1, 0))
F32 = jnp.float32
BF16 = jnp.bfloat16


def rms_norm(tokens, gamma_vec):
    tok_f32 = tokens.astype(F32)
    inv_rms = lax.rsqrt(jnp.mean(tok_f32 * tok_f32, axis=-1, keepdims=True) + EPS_NORM)
    return (tok_f32 * inv_rms * gamma_vec.astype(F32)).astype(BF16)


def rope_tables(seq_len, head_dim):
    half_dim = head_dim // 2
    steps = np.arange(half_dim, dtype=np.float32) * np.float32(2.0 / head_dim)
    inv_freq = np.power(np.float32(ROPE_BASE), -steps)
    angles = np.arange(seq_len, dtype=np.float32)[:, None] * inv_freq[None, :]
    cos_tab, sin_tab = np.cos(angles), np.sin(angles)
    return jnp.asarray(np.tile(cos_tab, (1, 4))), jnp.asarray(np.tile(np.concatenate([-sin_tab, sin_tab], axis=1), (1, 2)))


def lane_masks(rows):
    lane = lax.broadcasted_iota(jnp.int32, (rows, LANES), 1)
    return lane % 64 < 32, lane < 64


def turn(vals, cos_tab, sin_tab, low_half):
    partner = jnp.where(low_half, pltpu.roll(vals, 96, 1), pltpu.roll(vals, 32, 1))
    return vals * cos_tab + partner * sin_tab


def head_mean(vals, head_a):
    sum_a = jnp.sum(jnp.where(head_a, vals, 0.0), axis=1, keepdims=True)
    sum_b = jnp.sum(jnp.where(head_a, 0.0, vals), axis=1, keepdims=True)
    return jnp.where(head_a, sum_a, sum_b) * (1.0 / 64)


def rope_norm(vals, cos_tab, sin_tab, low_half, head_a):
    rotated = turn(vals.astype(F32), cos_tab, sin_tab, low_half)
    inv = lax.rsqrt(head_mean(rotated * rotated, head_a) + EPS_QK)
    return rotated, inv, (rotated * inv).astype(BF16)


def rope_norm_back(d_out, rotated, inv, cos_tab, sin_tab, low_half, head_a):
    d_rot = inv * d_out - rotated * (inv * inv * inv * head_mean(d_out * rotated, head_a))
    return turn(d_rot, cos_tab, -sin_tab, low_half).astype(BF16)


def dot_nn(lhs, rhs):
    return jnp.einsum('ik,kj->ij', lhs, rhs, preferred_element_type=F32)


def dot_nt(lhs, rhs):
    return jnp.einsum('ik,jk->ij', lhs, rhs, preferred_element_type=F32)


def dot_tn(lhs, rhs):
    return jnp.einsum('ki,kj->ij', lhs, rhs, preferred_element_type=F32)


def softmax_block(q_rows, k_all, start, keys):
    scores = dot_nt(q_rows, k_all[:keys]) * 0.125
    row = start + lax.broadcasted_iota(jnp.int32, scores.shape, 0)
    col = lax.broadcasted_iota(jnp.int32, scores.shape, 1)
    scores = jnp.where(row >= col, scores, -1e30)
    weights = jnp.exp(scores - jnp.max(scores, axis=1, keepdims=True))
    return weights / jnp.sum(weights, axis=1, keepdims=True)


def attn_fwd_kernel(q_ref, k_ref, v_ref, cos_ref, sin_ref, o_ref):
    seq = q_ref.shape[0]
    low_half, head_a = lane_masks(seq)
    cos_tab, sin_tab = cos_ref[:], sin_ref[:]
    q_rot = rope_norm(q_ref[:], cos_tab, sin_tab, low_half, head_a)[-1]
    k_rot = rope_norm(k_ref[:], cos_tab, sin_tab, low_half, head_a)[-1]
    v_all = v_ref[:]
    zero = jnp.zeros_like(q_rot)
    q_heads = jnp.where(head_a, q_rot, zero), jnp.where(head_a, zero, q_rot)
    for start in range(0, seq, QUERY_BLOCK):
        keys = start + QUERY_BLOCK
        outs = [dot_nn(softmax_block(q_head[start:keys], k_rot, start, keys).astype(BF16), v_all[:keys]) for q_head in q_heads]
        o_ref[start:keys, :] = jnp.where(head_a[:QUERY_BLOCK], outs[0], outs[1]).astype(BF16)


def attn_bwd_kernel(q_ref, k_ref, v_ref, do_ref, cos_ref, sin_ref, d_ref):
    seq = q_ref.shape[0]
    low_half, head_a = lane_masks(seq)
    cos_tab, sin_tab = cos_ref[:], sin_ref[:]
    q_raw, q_inv, q_rot = rope_norm(q_ref[:], cos_tab, sin_tab, low_half, head_a)
    k_raw, k_inv, k_rot = rope_norm(k_ref[:], cos_tab, sin_tab, low_half, head_a)
    v_all, d_o = v_ref[:], do_ref[:]
    zero = jnp.zeros_like(q_rot)
    grads = []
    for head in range(2):
        def only(vals, head=head):
            return jnp.where(head_a, vals, zero) if head == 0 else jnp.where(head_a, zero, vals)

        q_head, do_head = only(q_rot), only(d_o)
        dq_rows, dk_sum, dv_sum = [], None, None
        for start in range(0, seq, QUERY_BLOCK):
            keys = start + QUERY_BLOCK
            probs = softmax_block(q_head[start:keys], k_rot, start, keys)
            d_probs = dot_nt(do_head[start:keys], v_all[:keys])
            d_scores = probs * (d_probs - jnp.sum(probs * d_probs, axis=1, keepdims=True)) * 0.125
            d_scores = d_scores.astype(BF16)
            dq_rows.append(dot_nn(d_scores, k_rot[:keys]))
            dk_part = dot_tn(d_scores, q_head[start:keys])
            dv_part = dot_tn(probs.astype(BF16), do_head[start:keys])
            if keys < seq:
                pad = jnp.zeros((seq - keys, LANES), F32)
                dk_part, dv_part = jnp.concatenate([dk_part, pad]), jnp.concatenate([dv_part, pad])
            dk_sum = dk_part if dk_sum is None else dk_sum + dk_part
            dv_sum = dv_part if dv_sum is None else dv_sum + dv_part
        grads.append((jnp.concatenate(dq_rows), dk_sum, dv_sum))
    d_q, d_k, d_v = (jnp.where(head_a, part_a, part_b) for part_a, part_b in zip(*grads))
    rotary = (cos_tab, sin_tab, low_half, head_a)
    parts = rope_norm_back(d_q, q_raw, q_inv, *rotary), rope_norm_back(d_k, k_raw, k_inv, *rotary), d_v.astype(BF16)
    for part, value in enumerate(parts):
        block = column_block(pl.program_id(0), part)
        d_ref[:, pl.ds(pl.multiple_of(block * LANES, LANES), LANES)] = value


def column_block(pair, part):
    return pair // 3 * 9 + part * 3 + pair % 3


def qkv_kernel(x_ref, gamma_ref, w_ref, qkv_ref, n_ref):
    @pl.when(pl.program_id(0) == 0)
    def _():
        n_ref[:] = rms_norm(x_ref[:], gamma_ref[:])

    qkv_ref[:] = dot_nn(n_ref[:], w_ref[:]).astype(BF16)


def norm_qkv(tokens, gamma, weights):
    (tok, dim), width = tokens.shape, weights.shape[1] // 8
    return pl.pallas_call(
        qkv_kernel, grid=(6,), in_specs=[fixed(tok, dim), fixed(1, dim), pl.BlockSpec((dim, width), lambda step: (0, step + step // 3))],
        out_specs=[pl.BlockSpec((tok, width), lambda step: (0, step)), fixed(tok, dim)],
        out_shape=[jax.ShapeDtypeStruct((tok, 6 * width), BF16), jax.ShapeDtypeStruct((tok, dim), BF16)],
        compiler_params=pltpu.CompilerParams(vmem_limit_bytes=VMEM_LIMIT),
        cost_estimate=kernel_cost(12 * tok * dim * width, dim * width),
    )(tokens, gamma, weights)


def fixed(*shape):
    return pl.BlockSpec(shape, lambda *_: (0,) * len(shape))


def kernel_cost(flops, moved):
    return pl.CostEstimate(flops=flops, bytes_accessed=moved, transcendentals=0)


def attn_call(kernel, name_cost, qkv, d_o, cos_tab, sin_tab, out_spec, out_width):
    seq = qkv.shape[0]
    head_specs = [pl.BlockSpec((seq, LANES), lambda pair, part=part: (0, column_block(pair, part))) for part in range(3)]
    table = fixed(seq, LANES)
    extra = [] if d_o is None else [pair_spec(seq)]
    return pl.pallas_call(
        kernel, grid=(6,), in_specs=head_specs + extra + [table, table], out_specs=out_spec, out_shape=jax.ShapeDtypeStruct((seq, out_width), BF16),
        compiler_params=pltpu.CompilerParams(vmem_limit_bytes=VMEM_LIMIT), cost_estimate=kernel_cost(name_cost * seq * seq * seq, qkv.size),
    )(qkv, qkv, qkv, *([] if d_o is None else [d_o]), cos_tab, sin_tab)


def pair_spec(seq):
    return pl.BlockSpec((seq, LANES), lambda pair: (0, pair))


def route_slots(flat_ids, n_experts, capacity):
    onehot = flat_ids[:, None] == jnp.arange(n_experts)[None, :]
    token = jnp.arange(flat_ids.size)
    before = (token[:, None] > token[None, :]).astype(BF16)
    running = jnp.dot(before, onehot.astype(BF16), preferred_element_type=F32)
    slot_idx = jnp.sum(jnp.where(onehot, running, 0.0), axis=1).astype(jnp.int32)
    return onehot, flat_ids * capacity + slot_idx


def hop(block, axis):
    return lax.ppermute(block, axis, SWAP)


def z_hop(block, step):
    return lax.ppermute(block, 'z', [(z_idx, z_idx ^ step) for z_idx in range(QUAD)])


def pick(array, idx, axis):
    return lax.dynamic_index_in_dim(array, idx, axis, keepdims=False)


def in_core_order(mine, other, axis):
    first = lax.axis_index('c') == 0
    return jnp.concatenate([jnp.where(first, mine, other), jnp.where(first, other, mine)], axis=axis)


def core_halves(array, axis):
    low, high = jnp.split(array, 2, axis=axis)
    first = lax.axis_index('c') == 0
    return jnp.where(first, low, high), jnp.where(first, high, low)


def plane_first(block):
    return block, hop(block, 'x'), hop(block, 'y')


def plane_pieces(first):
    block, from_x, from_y = first
    half = block.shape[0] // 2
    return block, from_x, from_y, hop(from_y[:half], 'x'), hop(from_x[half:], 'y')


def after(value, *anchors):
    return lax.optimization_barrier((value,) + anchors)[0]


def z_stack(parts, gate):
    half = parts[0].shape[1] // 2
    c_me = lax.axis_index('c')

    def side(core):
        return jnp.concatenate([lax.dynamic_slice_in_dim(part, core * half, half, axis=1) for part in parts], axis=1)

    chip = after(in_core_order(side(c_me), hop(side(1 - c_me), 'c'), 0), gate)
    return [chip] + [z_hop(chip, step) for step in Z_STEPS]


def weight_kernel(att_ref, small_ref, att_out, small_out, local_sems, send_sems, recv_sems):
    z_me, y_me, x_me, c_me = (lax.axis_index(name) for name in AXES)
    peers = [((z_me + step) % 4, y_me, x_me, c_me) for step in Z_STEPS]
    peer_x, peer_y, peer_c = (z_me, y_me, 1 - x_me, c_me), (z_me, 1 - y_me, x_me, c_me), (z_me, y_me, x_me, 1 - c_me)
    barrier = pltpu.get_barrier_semaphore()
    everyone = peers + [peer_x, peer_y, peer_c]
    for peer in everyone:
        pl.semaphore_signal(barrier, inc=1, device_id=peer, device_id_type=pl.DeviceIdType.MESH)
    pl.semaphore_wait(barrier, len(everyone))

    def slot(back, rel, core):
        y_at, x_at = (1 - y_me if rel >= 2 else y_me), (1 - x_me if rel % 2 else x_me)
        return (((z_me + 4 - back) % 4 * 2 + y_at) * 2 + x_at) * 2 + core

    pairs = ((att_ref, att_out), (small_ref, small_out))

    started = []

    def send(back, rel, peer, sem, own=False):
        at = slot(back, rel, c_me)
        for kind, (src, out) in enumerate(pairs):
            copy = pltpu.make_async_remote_copy(
                src_ref=src if own else out.at[at], dst_ref=out.at[at], send_sem=send_sems.at[kind, sem], recv_sem=recv_sems.at[kind, sem],
                device_id=peer, device_id_type=pl.DeviceIdType.MESH)
            copy.start()
            started.append(copy)

    def landed(back, rel, sem, core=c_me):
        for kind, (src, out) in enumerate(pairs):
            pltpu.make_async_copy(src, out.at[slot(back, rel, core)], recv_sems.at[kind, sem]).wait()

    z_sem, x_sem, y_sem, far_sem, c_sem = range(0, 20, 4)
    for step, peer in zip(Z_STEPS, peers):
        send(0, 0, peer, z_sem + step, own=True)
    for back in range(QUAD):
        if back:
            landed(back, 0, z_sem + back)
        send(back, 0, peer_x, x_sem + back, own=not back)
        send(back, 0, peer_y, y_sem + back, own=not back)
        send(back, 0, peer_c, c_sem + QUAD * back, own=not back)
    for back in range(QUAD):
        landed(back, 1, x_sem + back)
        if back >= 2:
            send(back, 1, peer_y, far_sem + back)
        send(back, 1, peer_c, c_sem + QUAD * back + 1)
        landed(back, 2, y_sem + back)
        if back < 2:
            send(back, 2, peer_x, far_sem + back)
        send(back, 2, peer_c, c_sem + QUAD * back + 2)
    for back in range(QUAD):
        landed(back, 3, far_sem + back)
        send(back, 3, peer_c, c_sem + QUAD * back + 3)
    local = [pltpu.make_async_copy(src, out.at[slot(0, 0, c_me)], local_sems.at[kind]) for kind, (src, out) in enumerate(pairs)]
    for copy in local:
        copy.start()
    for back in range(QUAD):
        for rel in range(QUAD):
            landed(back, rel, c_sem + QUAD * back + rel, 1 - c_me)
    for copy in local:
        copy.wait()
    for copy in started:
        copy.wait_send()


def gather_weights(att_block, small):
    any_spec = pl.BlockSpec(memory_space=pl.ANY)
    blocks = (att_block, small)
    return pl.pallas_call(
        weight_kernel, in_specs=[any_spec] * 2, out_specs=[any_spec] * 2,
        out_shape=[jax.ShapeDtypeStruct((32,) + block.shape, block.dtype) for block in blocks],
        scratch_shapes=[pltpu.SemaphoreType.DMA((2,)), pltpu.SemaphoreType.DMA((2, 32)), pltpu.SemaphoreType.DMA((2, 32))],
        compiler_params=pltpu.CompilerParams(collective_id=0, has_side_effects=True),
        cost_estimate=kernel_cost(att_block.size * 10 ** 5, att_block.size),
    )(*blocks)


def expert_chips(w1_expert, w3_expert, w2_expert):
    c_me = lax.axis_index('c')
    up = jnp.stack([w1_expert, w3_expert])
    up_chip = in_core_order(pick(up, c_me, 1), hop(pick(up, 1 - c_me, 1), 'c'), 1)
    down_chip = in_core_order(pick(w2_expert, c_me, 0), hop(pick(w2_expert, 1 - c_me, 0), 'c'), 0)
    return up_chip, down_chip.reshape(2, -1, down_chip.shape[1])


def dot32(lhs, rhs):
    return jnp.dot(lhs, rhs, preferred_element_type=F32)


def ffn_rows(rows_ref, dd_ref, w1_ref, w3_ref, w2_ref, w2_turned, wait_w2, act_ref, dg_ref, dl_ref, out_acc, back_acc):
    chunk = 512

    def step(idx, carry):
        at = pl.ds(pl.multiple_of(idx * chunk, chunk), chunk)
        gate, lin = dot_nn(rows_ref[at, :], w1_ref[:]), dot_nn(rows_ref[at, :], w3_ref[:])
        sig = jax.nn.sigmoid(gate)
        silu = gate * sig
        act = (silu * lin).astype(BF16)
        act_ref[at, :] = act
        if wait_w2 is not None:
            wait_w2(idx)
        w2 = w2_ref[:]
        d_act = (dot_nn(dd_ref[at, :], w2) if w2_turned else dot_nt(dd_ref[at, :], w2)).astype(BF16).astype(F32)
        d_lin = (d_act * silu).astype(BF16)
        d_gate = (d_act * lin * (sig + silu * (1.0 - sig))).astype(BF16)
        dg_ref[at, :] = d_gate
        dl_ref[at, :] = d_lin
        out_acc[at, :] += dot_nt(act, w2) if w2_turned else dot_nn(act, w2)
        back_acc[at, :] += dot_nt(d_gate, w1_ref[:]) + dot_nt(d_lin, w3_ref[:])
        return carry

    lax.fori_loop(0, rows_ref.shape[0] // chunk, step, 0)


def row_grads(lhs_s, grad, away, near, x_first):
    for slot in range(2):
        away[slot] = dot_nn(lhs_s[2 * slot + 1 if x_first else slot + 2], grad[:])
        near[slot] = dot_nn(lhs_s[2 * slot if x_first else slot], grad[:])


def expert_kernel(half, info, rows_ref, dd_ref, rows_t_ref, dd_t_ref, *refs):
    up_refs, down_refs, refs = refs[:8], refs[8:13], refs[13:]
    if half == 1:
        acc_in, refs = refs[:2], refs[2:]
    out_ref, back_ref, g1_away, g1_near, g3_away, g3_near, g2_away, g2_near = refs[:8]
    w1, w3, w2, act_s, dg_s, dl_s, out_acc, back_acc, lhs_s, sems = refs[8:]
    step, me = pl.program_id(0), info[0]
    same_y = (me // 2) == half
    pieces = [(ref.at[0], ref.at[1]) for ref in down_refs[:3]] + [[ref.at[0] for ref in down_refs[3:]]]
    w2_halves = [w2.at[pl.ds(part * 384, 384)] for part in range(2)]
    for rel, srcs in enumerate(pieces):
        @pl.when(jnp.logical_and(same_y == (rel < 2), (step == 0) == (rel % 2 == 1)))
        def _(srcs=srcs):
            for part, src in enumerate(srcs):
                pltpu.make_async_copy(src, w2_halves[part], sems.at[part]).start()

    @pl.when(step == 0)
    def _():
        if half == 1:
            out_acc[:] = acc_in[0][:]
            back_acc[:] = acc_in[1][:]
        else:
            out_acc[:] = jnp.zeros_like(out_acc)
            back_acc[:] = jnp.zeros_like(back_acc)
        for rel in range(QUAD):
            lhs_s[rel] = rows_t_ref[pl.ds(pl.multiple_of((me ^ rel) * 192, 64), 192), :]

    for rel in range(QUAD):
        at = pl.ds(pl.multiple_of((me ^ rel) * 192, 64), 192)
        w1[at, :] = up_refs[rel][0]
        w3[at, :] = up_refs[4 + rel][0]

    def wait_w2(idx):
        @pl.when(idx == 0)
        def _():
            for part, src in enumerate(pieces[0]):
                pltpu.make_async_copy(src, w2_halves[part], sems.at[part]).wait()

    ffn_rows(rows_ref, dd_ref, w1, w3, w2, False, wait_w2, act_s, dg_s, dl_s, out_acc, back_acc)
    row_grads(lhs_s, dg_s, g1_away, g1_near, True)
    row_grads(lhs_s, dl_s, g3_away, g3_near, False)

    for near in range(2):
        @pl.when(step == near)
        def _(g2_ref=(g2_away, g2_near)[near]):
            for part in range(2):
                at = slice(part * 384, part * 384 + 384)
                g2_ref[at, :] = dot_nn(dd_t_ref[at, :], act_s[:])

    @pl.when(step == 1)
    def _():
        out_ref[:] = out_acc[:].astype(out_ref.dtype)
        back_ref[:] = back_acc[:].astype(back_ref.dtype)


def expert_half(half, rows, dd, rows_t, dd_t, up, down, acc):
    tok, dim = rows.shape
    y_me, x_me = lax.axis_index('y'), lax.axis_index('x')
    info = jnp.stack([2 * y_me + x_me, 2 * half + 1 - x_me, 2 * half + x_me]).astype(jnp.int32)
    whole, turned = fixed(tok, dim), fixed(dim, tok)

    def up_spec(mat):
        return pl.BlockSpec((1, dim // QUAD, dim), lambda step, info_ref, mat=mat: (mat, 0, info_ref[1 + step]))

    own, from_x, from_y, low, high = up
    up_args = (own, from_x, from_y, low, own, from_x, from_y, high)
    up_specs = [up_spec(0)] * QUAD + [up_spec(1)] * 3 + [up_spec(0)]
    any_spec = pl.BlockSpec(memory_space=pl.ANY)
    row_out = pl.BlockSpec((2, dim // QUAD, dim), lambda step, info_ref: (0, 0, info_ref[1 + step] - 2 * half))
    square = fixed(dim, dim)
    acc_type = F32 if half == 0 else BF16
    row_shape, square_shape = jax.ShapeDtypeStruct((2, dim // QUAD, 2 * dim), F32), jax.ShapeDtypeStruct((dim, dim), F32)
    return pl.pallas_call(
        lambda *refs: expert_kernel(half, *refs),
        grid_spec=pltpu.PrefetchScalarGridSpec(
            num_scalar_prefetch=1, grid=(2,),
            in_specs=[whole, whole, turned, turned] + up_specs + [any_spec] * 5 + [whole] * len(acc),
            out_specs=[whole, whole] + [row_out] * QUAD + [square] * 2,
            scratch_shapes=[pltpu.VMEM((dim, dim), BF16)] * 3 + [pltpu.VMEM((tok, dim), BF16)] * 3 + [pltpu.VMEM((tok, dim), F32)] * 2 + [pltpu.VMEM((QUAD, dim // QUAD, tok), BF16), pltpu.SemaphoreType.DMA((2,))]),
        out_shape=[jax.ShapeDtypeStruct((tok, dim), acc_type)] * 2 + [row_shape] * QUAD + [square_shape] * 2,
        compiler_params=pltpu.CompilerParams(vmem_limit_bytes=VMEM_LIMIT),
        cost_estimate=kernel_cost(36 * tok * dim * dim, dim * dim),
    )(info, rows, dd, rows_t, dd_t, *up_args, *down, *acc)


def shared_kernel(info, rows_ref, dd_ref, rows_t_ref, dd_t_ref, *refs):
    pieces, refs = [refs[5 * mat:5 * mat + 5] for mat in range(3)], refs[15:]
    out_refs, back_refs, g3_away, g3_near, g1_refs, g2_refs = refs[:2], refs[2:4], refs[4], refs[5], refs[6:10], refs[10:14]
    w1, w3, w2, act_s, dg_s, dl_s, out_acc, back_acc, lhs_s, lhs_z, dd_z = refs[14:]
    step, me, z_me = pl.program_id(0), info[0], info[1]

    def spot(rel, turn_z):
        return pl.ds(pl.multiple_of(((z_me ^ turn_z) * QUAD + (me ^ rel)) * ROWS, 16), ROWS)

    @pl.when(step == 0)
    def _():
        out_acc[:] = jnp.zeros_like(out_acc)
        back_acc[:] = jnp.zeros_like(back_acc)
        for rel in range(QUAD):
            for turn_z in range(QUAD):
                inner = slice(rel * ROWS, rel * ROWS + ROWS)
                lhs_s[rel, turn_z * ROWS:turn_z * ROWS + ROWS, :] = rows_t_ref[spot(rel, turn_z), :]
                lhs_z[turn_z, inner, :] = rows_t_ref[spot(rel, turn_z), :]
                dd_z[turn_z, inner, :] = dd_t_ref[spot(rel, turn_z), :]

    for w_ref, (own, from_x, from_y, low, high) in zip((w1, w3, w2), pieces):
        for turn_z in range(QUAD):
            for rel, src in enumerate((own.at[turn_z], from_x.at[turn_z], from_y.at[turn_z], low.at[turn_z] if turn_z < 2 else high.at[turn_z - 2])):
                w_ref[spot(rel, turn_z), :] = src[:]

    ffn_rows(rows_ref, dd_ref, w1, w3, w2, True, None, act_s, dg_s, dl_s, out_acc, back_acc)
    row_grads(lhs_s, dl_s, g3_away, g3_near, False)
    for turn_z in range(QUAD):
        g1_refs[turn_z][:] = dot_nn(lhs_z[turn_z], dg_s[:])
        g2_refs[turn_z][:] = dot_nn(dd_z[turn_z], act_s[:])

    @pl.when(step == pl.num_programs(0) - 1)
    def _():
        for acc, halves in ((out_acc, out_refs), (back_acc, back_refs)):
            for ref, value in zip(halves, jnp.split(acc[:], 2, axis=0)):
                ref[:] = value


def shared_ffn(gate, rows, dd, rows_t, dd_t, pieces):
    tok, dim = rows.shape
    width = pieces[0].shape[2] // 3
    steps = width // dim
    info = after(jnp.stack([2 * lax.axis_index('y') + lax.axis_index('x'), lax.axis_index('z')]).astype(jnp.int32), gate)
    whole, turned, half = fixed(tok, dim), fixed(dim, tok), fixed(tok // 2, dim)
    piece_specs = [pl.BlockSpec((piece.shape[0], ROWS, dim), lambda step, info_ref, mat=mat: (0, 0, mat * steps + step)) for mat in range(3) for piece in pieces]
    row_out = pl.BlockSpec((2, dim // QUAD, dim), lambda step, info_ref: (0, 0, step))
    z_out = pl.BlockSpec((dim // QUAD, dim), lambda step, info_ref: (0, step))
    shapes = ((tok // 2, dim),) * QUAD + ((2, dim // QUAD, width),) * 2 + ((dim // QUAD, width),) * 8
    outs = pl.pallas_call(
        shared_kernel,
        grid_spec=pltpu.PrefetchScalarGridSpec(
            num_scalar_prefetch=1, grid=(steps,),
            in_specs=[whole, whole, turned, turned] + piece_specs,
            out_specs=[half] * QUAD + [row_out] * 2 + [z_out] * 8,
            scratch_shapes=[pltpu.VMEM((dim, dim), BF16)] * 3 + [pltpu.VMEM((tok, dim), BF16)] * 3 + [pltpu.VMEM((tok, dim), F32)] * 2 + [pltpu.VMEM((QUAD, dim // QUAD, tok), BF16)] * 3),
        out_shape=[jax.ShapeDtypeStruct(shape, F32) for shape in shapes],
        compiler_params=pltpu.CompilerParams(vmem_limit_bytes=VMEM_LIMIT),
        cost_estimate=kernel_cost(18 * tok * dim * width, dim * width),
    )(info, rows, dd, rows_t, dd_t, *(list(pieces) * 3))
    return outs[:2], outs[2:4], outs[4:6], outs[6:10], outs[10:]


def z_sum(plane):
    summed = plane[0]
    for step in (1, 2, 3):
        summed = summed + z_hop(plane[step], step)
    return summed


def swap_rows(summed):
    halves = summed.reshape(summed.shape[:-2] + (2, -1, summed.shape[-1]))
    axis, c_me = halves.ndim - 3, lax.axis_index('c')
    return pick(halves, c_me, axis), hop(pick(halves, 1 - c_me, axis), 'c')


def plane_sum_values(total):
    y_me, x_me = lax.axis_index('y'), lax.axis_index('x')
    ways = tuple(zip((total[:2], total[2:]), ((2, x_me, y_me, 'x', 'y'), (1, y_me, x_me, 'y', 'x'))))
    gives = [pick(part, 1 - me_1, axis_1) for part, (axis_1, me_1, *_) in ways]

    def rest():
        planes = []
        for give, (part, (axis_1, me_1, me_2, name_1, name_2)) in zip(gives, ways):
            got, keep = hop(give, name_1), pick(part, me_1, axis_1)
            got_2 = hop(pick(keep, 1 - me_2, 1) + pick(got, 1 - me_2, 1), name_2)
            planes.append(pick(keep, me_2, 1) + pick(got, me_2, 1) + got_2)
        return jnp.concatenate(planes, axis=0)

    return gives, rest


def swap_experts(summed):
    return in_core_order(*(part[None] for part in swap_rows(summed)), 0)


def layer_step(x_in, grad_y, w_q, w_k, w_v, w_o, gamma_attn, gamma_mlp, w_router, w1_shared, w3_shared, w2_shared, w1_expert, w3_expert, w2_expert, expert_ids):
    n_batch, seq_len, model_dim = x_in.shape
    n_tok = n_batch * seq_len
    n_heads, head_dim = w_q.shape[1], w_q.shape[2]
    att_dim, att_half = n_heads * head_dim, n_heads * head_dim // 2
    n_experts = w_router.shape[1]
    ff_half = w1_shared.shape[1] // 2
    capacity = 2 * n_tok // n_experts
    n_slots = n_experts * capacity

    att_parts = (w_q.reshape(-1, att_dim), w_k.reshape(-1, att_dim), w_v.reshape(-1, att_dim), w_o.reshape(att_dim, -1).T)
    att_block = jnp.concatenate([part[:, :att_half] for part in att_parts] + [part[:, att_half:] for part in att_parts], axis=1)
    small = jnp.concatenate([gamma_attn.astype(F32)[:, None], gamma_mlp.astype(F32)[:, None], w_router], axis=1)
    small = jnp.pad(small, ((0, 0), (0, LANES - small.shape[1])))
    up_chip, down_chip = expert_chips(w1_expert, w3_expert, w2_expert)
    att_all, small_all = gather_weights(att_block, small)
    att_all, small_all = att_all.reshape(model_dim, -1), small_all.reshape(model_dim, -1)
    ga_all, gm_all, wr_all = small_all[:, 0], small_all[:, 1], small_all[:, 2:2 + n_experts]
    down_first = plane_first(down_chip)
    up_first = plane_first(up_chip)
    sh_parts = z_stack((w1_shared, w3_shared, w2_shared.T), small_all)

    d_out = grad_y.reshape(n_tok, model_dim)
    onehot, dest_row = route_slots(expert_ids.reshape(n_tok), n_experts, capacity)
    place = (dest_row[:, None] == jnp.arange(n_slots)[None, :]).astype(BF16)

    def exchange(values):
        return lax.all_to_all(values.reshape(n_experts, capacity, model_dim), ('z', 'c'), 0, 0, tiled=True).reshape(n_slots, model_dim)

    def dispatch(values):
        return jnp.einsum('ts,td->sd', place, values, preferred_element_type=F32).astype(BF16)

    d_out_both = jnp.concatenate([d_out, hop(d_out, 'c')], axis=0)
    d_out_t = d_out_both.T
    tables = rope_tables(seq_len, head_dim)

    tokens = x_in.reshape(n_tok, model_dim)
    qkv, normed1 = norm_qkv(tokens, ga_all[None, :], att_all)
    norm1_pull = jax.vjp(rms_norm, tokens, ga_all)[1]
    heads = attn_call(attn_fwd_kernel, 8, qkv, None, *tables, pair_spec(n_tok), att_dim)
    half_cols = [slice(start, start + att_half) for start in (0, att_half)]
    wot = [att_all[:, start + 3 * att_half:start + QUAD * att_half] for start in (0, QUAD * att_half)]
    attn_out = sum(jnp.einsum('tk,dk->td', heads[:, cols], w_half, preferred_element_type=F32) for cols, w_half in zip(half_cols, wot))
    hidden = (tokens.astype(F32) + attn_out).astype(BF16)
    normed2, norm2_pull = jax.vjp(rms_norm, hidden, gm_all)
    normed2_f = normed2.astype(F32)
    logits = jnp.dot(normed2, wr_all, preferred_element_type=F32, precision=lax.Precision.HIGHEST)
    gate_val = jax.nn.sigmoid(jnp.sum(jnp.where(onehot, logits, 0.0), axis=1))
    routed_in = (gate_val[:, None] * normed2_f).astype(BF16)
    give_r = dispatch(routed_in)
    give_d = dispatch(after(d_out, give_r))
    rows = exchange(give_r)
    d_down = exchange(after(give_d, rows))
    rows_t, d_down_t = rows.T, d_down.T

    normed2_both = jnp.concatenate([normed2, hop(normed2, 'c')], axis=0)
    normed2_t = normed2_both.T
    sh_first = plane_first(jnp.stack([after(part, heads) for part in sh_parts]))

    def settle(pieces):
        return [after(piece, give_r, give_d, normed2_t, d_out_t) for piece in pieces]

    sh_pieces = plane_pieces(settle(sh_first))
    down_pieces = plane_pieces(settle(down_first))
    up_pieces = plane_pieces(settle(up_first))
    shared_part, d_part, (s3_away, s3_near), s1, s2 = shared_ffn(rows_t, normed2_both, d_out_both, normed2_t, d_out_t, sh_pieces)
    shared_out = shared_part[0] + hop(shared_part[1], 'c')
    d_normed2 = d_part[0] + hop(d_part[1], 'c')

    *acc, a1_away, a1_near, a3_away, a3_near, a2_away, a2_near = expert_half(0, rows, d_down, rows_t, d_down_t, up_pieces, down_pieces, ())
    down_rows, d_rows, b1_away, b1_near, b3_away, b3_near, b2_away, b2_near = expert_half(1, rows, d_down, rows_t, d_down_t, up_pieces, down_pieces, acc)
    d_back = exchange(d_rows)

    def first_sum(away, near, axis, gate):
        keep, give = near + after(hop(away, axis), *gate)
        return keep, hop(give, 'y' if axis == 'x' else 'x')

    s3 = first_sum(s3_away, s3_near, 'y', [d_rows])
    a1, a3 = first_sum(a1_away, a1_near, 'x', [d_rows]), first_sum(a3_away, a3_near, 'y', [d_rows])
    d_routed_in = jnp.einsum('ts,sd->td', place, d_back, preferred_element_type=F32)
    d_normed2 = d_normed2 + gate_val[:, None] * d_routed_in
    d_gate_val = jnp.sum(d_routed_in * normed2_f, axis=1) * gate_val * (1.0 - gate_val)
    d_logits = jnp.where(onehot, d_gate_val[:, None], 0.0)
    g_wr = jnp.einsum('td,te->de', normed2_f, d_logits, precision=lax.Precision.HIGHEST)
    d_normed2 = d_normed2 + jnp.einsum('te,de->td', d_logits, wr_all, precision=lax.Precision.HIGHEST)
    d_hid_norm, g_gm = norm2_pull(d_normed2.astype(BF16))
    d_hidden = (d_out.astype(F32) + d_hid_norm.astype(F32)).astype(BF16)

    d_hidden_t, normed1_t = d_hidden.T, normed1.T
    d_heads = jnp.concatenate([dot32(d_hidden, w_half).astype(BF16) for w_half in wot], axis=1)
    d_qkv = attn_call(attn_bwd_kernel, 16, qkv, d_heads, *tables, fixed(n_tok, 3 * att_dim), 3 * att_dim)
    d_halves = jnp.split(d_qkv, 2, axis=1)
    d_normed1 = sum(jnp.einsum('tk,dk->td', half, att_all[:, start:start + 3 * att_half], preferred_element_type=F32) for half, start in zip(d_halves, (0, QUAD * att_half)))
    d_tok_norm, g_ga = norm1_pull(d_normed1.astype(BF16))
    g_small = jnp.concatenate([g_ga[:, None], g_gm[:, None], g_wr, jnp.zeros((model_dim, 6), F32)], axis=1)
    core_0 = lax.axis_index('c') == 0

    def core_pick(pair):
        first, second = pair
        return jnp.where(core_0, first, second), jnp.where(core_0, second, first)

    g_att = []
    for lhs_t, pair in ((normed1_t, d_halves), (d_hidden_t, [heads[:, cols] for cols in half_cols])):
        mine, other = core_pick(pair)
        g_att.append(dot32(lhs_t, mine) + hop(dot32(lhs_t, other), 'c'))
    mine, other = (jnp.pad(half, ((0, 0), (0, LANES - half.shape[1]))) for half in core_pick(jnp.split(g_small, 2, axis=1)))
    g_att.append(mine + hop(other, 'c'))
    att_gives, att_rest = plane_sum_values(jnp.concatenate(g_att, axis=1).reshape(QUAD, 2, 2, ROWS, -1))

    def later(value):
        return after(value, *att_gives)

    low_y = lax.axis_index('y') == 0
    g2_low, g2_high = a2_near + later(hop(a2_away, 'x')), b2_near + later(hop(b2_away, 'x'))
    g2_keep, g2_give = jnp.where(low_y, g2_low, g2_high), jnp.where(low_y, g2_high, g2_low)

    def z_first(parts):
        total = parts[0]
        for step in Z_STEPS:
            total = total + after(z_hop(parts[step], step), g2_give)
        return jnp.split(total.reshape(2, 2, ROWS, -1), 2, axis=1)

    def z_last(pair):
        keep, give = pair
        keep, give = keep + hop(give, 'x')
        return (keep + hop(give, 'y')).reshape(ROWS, -1)

    s1, s2 = z_first(s1), z_first(s2)
    b_gates = [s1[1], s2[1]]
    routed = jnp.einsum('ts,sd->td', place, exchange(later(down_rows)), preferred_element_type=F32)
    layer_out = (hidden.astype(F32) + routed + shared_out).astype(BF16)
    b1, b3 = first_sum(b1_away, b1_near, 'x', b_gates), first_sum(b3_away, b3_near, 'y', b_gates)

    def finish(pairs):
        return jnp.concatenate([mine + later(got) for mine, got in pairs], axis=1)

    g_w1, g_w3 = finish((a1, b1)), finish((a3, b3))
    g2_mine, g2_other = core_halves(g2_keep + hop(g2_give, 'y'), 1)
    g_w2e = in_core_order(g2_mine.T[None], hop(g2_other, 'c').T[None], 0)
    g_sh = jnp.concatenate([z_last(s1), z_sum(finish((s3,)).reshape(QUAD, ROWS, -1)), z_last(s2)], axis=1)
    g_sh_mine, g_sh_other = swap_rows(g_sh)
    g_up = swap_experts(jnp.stack([g_w1, g_w3]))
    z_me = lax.axis_index('z')
    att_plane = att_rest()
    g_att_mine, g_att_other = swap_rows(z_sum([pick(att_plane, z_me ^ step, 0) for step in range(QUAD)]))
    d_x = (d_hidden.astype(F32) + d_tok_norm.astype(F32)).astype(BF16).reshape(n_batch, seq_len, model_dim)

    g_small = in_core_order(*(part[:, QUAD * att_half:QUAD * att_half + 8] for part in (g_att_mine, g_att_other)), 1)
    g_att_mine, g_att_other = g_att_mine[:, :QUAD * att_half], g_att_other[:, :QUAD * att_half]
    g_att = in_core_order(g_att_mine.reshape(-1, QUAD, att_half), g_att_other.reshape(-1, QUAD, att_half), 2)
    g_q, g_k, g_v = (g_att[:, part].reshape(-1, n_heads, head_dim) for part in range(3))
    g_wo = g_att[:, 3].T.reshape(n_heads, head_dim, -1)
    g_sh = in_core_order(g_sh_mine.reshape(-1, 3, ff_half), g_sh_other.reshape(-1, 3, ff_half), 2)
    return (layer_out.reshape(n_batch, seq_len, model_dim), d_x, g_q, g_k, g_v, g_wo, g_small[:, 0], g_small[:, 1], g_small[:, 2:2 + n_experts], g_sh[:, 0], g_sh[:, 1], g_sh[:, 2].T, g_up[:, 0], g_up[:, 1], g_w2e)


def solution(mesh):
    fine_mesh = Mesh(np.asarray(mesh.devices).reshape(4, 2, 2, 2), AXES)
    row_spec, wo_spec, w2s_spec, exp_spec = P(AXES), P(None, None, AXES), P(None, AXES), P('z', AXES[1:])
    weight_specs = (row_spec,) * 3 + (wo_spec,) + (row_spec,) * 5 + (w2s_spec,) + (exp_spec,) * 3
    out_specs = (row_spec, row_spec) + weight_specs
    in_specs = out_specs + (row_spec,)
    return jax.shard_map(layer_step, mesh=fine_mesh, in_specs=in_specs, out_specs=out_specs, check_vma=False)
```

```python
import jax
import jax.numpy as jnp
import numpy as np
from jax import lax
from jax.experimental import pallas as pl
from jax.experimental.pallas import tpu as pltpu
from jax.sharding import Mesh, PartitionSpec as P

LANES = 128
ROWS = 48
QUAD = 4
EPS_NORM = 1e-5
EPS_QK = 1e-6
ROPE_BASE = 500000.0
QUERY_BLOCK = 256
VMEM_LIMIT = 60 * 1024 * 1024
AXES = ('z', 'y', 'x', 'c')
Z_STEPS = (1, 2, 3)
SWAP = ((0, 1), (1, 0))
F32 = jnp.float32
BF16 = jnp.bfloat16


def rms_norm(tokens, gamma_vec):
    tok_f32 = tokens.astype(F32)
    inv_rms = lax.rsqrt(jnp.mean(tok_f32 * tok_f32, axis=-1, keepdims=True) + EPS_NORM)
    return (tok_f32 * inv_rms * gamma_vec.astype(F32)).astype(BF16)


def rope_tables(seq_len, head_dim):
    half_dim = head_dim // 2
    steps = np.arange(half_dim, dtype=np.float32) * np.float32(2.0 / head_dim)
    inv_freq = np.power(np.float32(ROPE_BASE), -steps)
    angles = np.arange(seq_len, dtype=np.float32)[:, None] * inv_freq[None, :]
    cos_tab, sin_tab = np.cos(angles), np.sin(angles)
    return jnp.asarray(np.tile(cos_tab, (1, 4))), jnp.asarray(np.tile(np.concatenate([-sin_tab, sin_tab], axis=1), (1, 2)))


def lane_masks(rows):
    lane = lax.broadcasted_iota(jnp.int32, (rows, LANES), 1)
    return lane % 64 < 32, lane < 64


def turn(vals, cos_tab, sin_tab, low_half):
    partner = jnp.where(low_half, pltpu.roll(vals, 96, 1), pltpu.roll(vals, 32, 1))
    return vals * cos_tab + partner * sin_tab


def head_mean(vals, head_a):
    sum_a = jnp.sum(jnp.where(head_a, vals, 0.0), axis=1, keepdims=True)
    sum_b = jnp.sum(jnp.where(head_a, 0.0, vals), axis=1, keepdims=True)
    return jnp.where(head_a, sum_a, sum_b) * (1.0 / 64)


def rope_norm(vals, cos_tab, sin_tab, low_half, head_a):
    rotated = turn(vals.astype(F32), cos_tab, sin_tab, low_half)
    inv = lax.rsqrt(head_mean(rotated * rotated, head_a) + EPS_QK)
    return rotated, inv, (rotated * inv).astype(BF16)


def rope_norm_back(d_out, rotated, inv, cos_tab, sin_tab, low_half, head_a):
    d_rot = inv * d_out - rotated * (inv * inv * inv * head_mean(d_out * rotated, head_a))
    return turn(d_rot, cos_tab, -sin_tab, low_half).astype(BF16)


def dot_nn(lhs, rhs):
    return jnp.einsum('ik,kj->ij', lhs, rhs, preferred_element_type=F32)


def dot_nt(lhs, rhs):
    return jnp.einsum('ik,jk->ij', lhs, rhs, preferred_element_type=F32)


def dot_tn(lhs, rhs):
    return jnp.einsum('ki,kj->ij', lhs, rhs, preferred_element_type=F32)


def softmax_block(q_rows, k_all, start, keys):
    scores = dot_nt(q_rows, k_all[:keys]) * 0.125
    row = start + lax.broadcasted_iota(jnp.int32, scores.shape, 0)
    col = lax.broadcasted_iota(jnp.int32, scores.shape, 1)
    scores = jnp.where(row >= col, scores, -1e30)
    weights = jnp.exp(scores - jnp.max(scores, axis=1, keepdims=True))
    return weights / jnp.sum(weights, axis=1, keepdims=True)


def attn_fwd_kernel(q_ref, k_ref, v_ref, cos_ref, sin_ref, o_ref):
    seq = q_ref.shape[0]
    low_half, head_a = lane_masks(seq)
    cos_tab, sin_tab = cos_ref[:], sin_ref[:]
    q_rot = rope_norm(q_ref[:], cos_tab, sin_tab, low_half, head_a)[-1]
    k_rot = rope_norm(k_ref[:], cos_tab, sin_tab, low_half, head_a)[-1]
    v_all = v_ref[:]
    zero = jnp.zeros_like(q_rot)
    q_heads = jnp.where(head_a, q_rot, zero), jnp.where(head_a, zero, q_rot)
    for start in range(0, seq, QUERY_BLOCK):
        keys = start + QUERY_BLOCK
        outs = [dot_nn(softmax_block(q_head[start:keys], k_rot, start, keys).astype(BF16), v_all[:keys]) for q_head in q_heads]
        o_ref[start:keys, :] = jnp.where(head_a[:QUERY_BLOCK], outs[0], outs[1]).astype(BF16)


def attn_bwd_kernel(q_ref, k_ref, v_ref, do_ref, cos_ref, sin_ref, d_ref):
    seq = q_ref.shape[0]
    low_half, head_a = lane_masks(seq)
    cos_tab, sin_tab = cos_ref[:], sin_ref[:]
    q_raw, q_inv, q_rot = rope_norm(q_ref[:], cos_tab, sin_tab, low_half, head_a)
    k_raw, k_inv, k_rot = rope_norm(k_ref[:], cos_tab, sin_tab, low_half, head_a)
    v_all, d_o = v_ref[:], do_ref[:]
    zero = jnp.zeros_like(q_rot)
    grads = []
    for head in range(2):
        def only(vals, head=head):
            return jnp.where(head_a, vals, zero) if head == 0 else jnp.where(head_a, zero, vals)

        q_head, do_head = only(q_rot), only(d_o)
        dq_rows, dk_sum, dv_sum = [], None, None
        for start in range(0, seq, QUERY_BLOCK):
            keys = start + QUERY_BLOCK
            probs = softmax_block(q_head[start:keys], k_rot, start, keys)
            d_probs = dot_nt(do_head[start:keys], v_all[:keys])
            d_scores = probs * (d_probs - jnp.sum(probs * d_probs, axis=1, keepdims=True)) * 0.125
            d_scores = d_scores.astype(BF16)
            dq_rows.append(dot_nn(d_scores, k_rot[:keys]))
            dk_part = dot_tn(d_scores, q_head[start:keys])
            dv_part = dot_tn(probs.astype(BF16), do_head[start:keys])
            if keys < seq:
                pad = jnp.zeros((seq - keys, LANES), F32)
                dk_part, dv_part = jnp.concatenate([dk_part, pad]), jnp.concatenate([dv_part, pad])
            dk_sum = dk_part if dk_sum is None else dk_sum + dk_part
            dv_sum = dv_part if dv_sum is None else dv_sum + dv_part
        grads.append((jnp.concatenate(dq_rows), dk_sum, dv_sum))
    d_q, d_k, d_v = (jnp.where(head_a, part_a, part_b) for part_a, part_b in zip(*grads))
    rotary = (cos_tab, sin_tab, low_half, head_a)
    parts = rope_norm_back(d_q, q_raw, q_inv, *rotary), rope_norm_back(d_k, k_raw, k_inv, *rotary), d_v.astype(BF16)
    for part, value in enumerate(parts):
        block = column_block(pl.program_id(0), part)
        d_ref[:, pl.ds(pl.multiple_of(block * LANES, LANES), LANES)] = value


def column_block(pair, part):
    return pair // 3 * 9 + part * 3 + pair % 3


def qkv_kernel(x_ref, gamma_ref, w_ref, qkv_ref, n_ref):
    @pl.when(pl.program_id(0) == 0)
    def _():
        n_ref[:] = rms_norm(x_ref[:], gamma_ref[:])

    qkv_ref[:] = dot_nn(n_ref[:], w_ref[:]).astype(BF16)


def norm_qkv(tokens, gamma, weights):
    (tok, dim), width = tokens.shape, weights.shape[1] // 8
    return pl.pallas_call(
        qkv_kernel, grid=(6,), in_specs=[fixed(tok, dim), fixed(1, dim), pl.BlockSpec((dim, width), lambda step: (0, step + step // 3))],
        out_specs=[pl.BlockSpec((tok, width), lambda step: (0, step)), fixed(tok, dim)],
        out_shape=[jax.ShapeDtypeStruct((tok, 6 * width), BF16), jax.ShapeDtypeStruct((tok, dim), BF16)],
        compiler_params=pltpu.CompilerParams(vmem_limit_bytes=VMEM_LIMIT),
        cost_estimate=kernel_cost(12 * tok * dim * width, dim * width),
    )(tokens, gamma, weights)


def fixed(*shape):
    return pl.BlockSpec(shape, lambda *_: (0,) * len(shape))


def kernel_cost(flops, moved):
    return pl.CostEstimate(flops=flops, bytes_accessed=moved, transcendentals=0)


def attn_call(kernel, name_cost, qkv, d_o, cos_tab, sin_tab, out_spec, out_width):
    seq = qkv.shape[0]
    head_specs = [pl.BlockSpec((seq, LANES), lambda pair, part=part: (0, column_block(pair, part))) for part in range(3)]
    table = fixed(seq, LANES)
    extra = [] if d_o is None else [pair_spec(seq)]
    return pl.pallas_call(
        kernel, grid=(6,), in_specs=head_specs + extra + [table, table], out_specs=out_spec, out_shape=jax.ShapeDtypeStruct((seq, out_width), BF16),
        compiler_params=pltpu.CompilerParams(vmem_limit_bytes=VMEM_LIMIT), cost_estimate=kernel_cost(name_cost * seq * seq * seq, qkv.size),
    )(qkv, qkv, qkv, *([] if d_o is None else [d_o]), cos_tab, sin_tab)


def pair_spec(seq):
    return pl.BlockSpec((seq, LANES), lambda pair: (0, pair))


def route_slots(flat_ids, n_experts, capacity):
    onehot = flat_ids[:, None] == jnp.arange(n_experts)[None, :]
    token = jnp.arange(flat_ids.size)
    before = (token[:, None] > token[None, :]).astype(BF16)
    running = jnp.dot(before, onehot.astype(BF16), preferred_element_type=F32)
    slot_idx = jnp.sum(jnp.where(onehot, running, 0.0), axis=1).astype(jnp.int32)
    return onehot, flat_ids * capacity + slot_idx


def hop(block, axis):
    return lax.ppermute(block, axis, SWAP)


def z_hop(block, step):
    return lax.ppermute(block, 'z', [(z_idx, z_idx ^ step) for z_idx in range(QUAD)])


def pick(array, idx, axis):
    return lax.dynamic_index_in_dim(array, idx, axis, keepdims=False)


def core_sorted(mine, other):
    first = lax.axis_index('c') == 0
    return jnp.where(first, mine, other), jnp.where(first, other, mine)


def in_core_order(mine, other, axis):
    return jnp.concatenate(core_sorted(mine, other), axis=axis)


def core_halves(array, axis):
    low, high = jnp.split(array, 2, axis=axis)
    first = lax.axis_index('c') == 0
    return jnp.where(first, low, high), jnp.where(first, high, low)


def plane_near(halves):
    return [hop(half, 'x') for half in halves], [hop(half, 'y') for half in halves]


def after(value, *anchors):
    return lax.optimization_barrier((value,) + anchors)[0]


def z_parts(parts):
    half = parts[0].shape[1] // 2
    c_me = lax.axis_index('c')

    def side(core):
        return jnp.concatenate([lax.dynamic_slice_in_dim(part, core * half, half, axis=1) for part in parts], axis=1)

    chip = in_core_order(side(c_me), hop(side(1 - c_me), 'c'), 0)
    return [chip] + [z_hop(chip, step) for step in Z_STEPS]


def weight_kernel(att_ref, small_ref, att_out, small_out, local_sems, send_sems, recv_sems):
    z_me, y_me, x_me, c_me = (lax.axis_index(name) for name in AXES)
    peers = [((z_me + step) % 4, y_me, x_me, c_me) for step in Z_STEPS]
    peer_x, peer_y, peer_c = (z_me, y_me, 1 - x_me, c_me), (z_me, 1 - y_me, x_me, c_me), (z_me, y_me, x_me, 1 - c_me)
    barrier = pltpu.get_barrier_semaphore()
    everyone = peers + [peer_x, peer_y, peer_c]
    for peer in everyone:
        pl.semaphore_signal(barrier, inc=1, device_id=peer, device_id_type=pl.DeviceIdType.MESH)
    pl.semaphore_wait(barrier, len(everyone))

    def slot(back, rel, core):
        y_at, x_at = (1 - y_me if rel >= 2 else y_me), (1 - x_me if rel % 2 else x_me)
        return (((z_me + 4 - back) % 4 * 2 + y_at) * 2 + x_at) * 2 + core

    pairs = ((att_ref, att_out), (small_ref, small_out))

    started = []

    def send(back, rel, peer, sem, own=False):
        at = slot(back, rel, c_me)
        for kind, (src, out) in enumerate(pairs):
            copy = pltpu.make_async_remote_copy(
                src_ref=src if own else out.at[at], dst_ref=out.at[at], send_sem=send_sems.at[kind, sem], recv_sem=recv_sems.at[kind, sem],
                device_id=peer, device_id_type=pl.DeviceIdType.MESH)
            copy.start()
            started.append(copy)

    def landed(back, rel, sem, core=c_me):
        for kind, (src, out) in enumerate(pairs):
            pltpu.make_async_copy(src, out.at[slot(back, rel, core)], recv_sems.at[kind, sem]).wait()

    z_sem, x_sem, y_sem, far_sem, c_sem = range(0, 20, 4)
    for step, peer in zip(Z_STEPS, peers):
        send(0, 0, peer, z_sem + step, own=True)
    for back in range(QUAD):
        if back:
            landed(back, 0, z_sem + back)
        send(back, 0, peer_x, x_sem + back, own=not back)
        send(back, 0, peer_y, y_sem + back, own=not back)
        send(back, 0, peer_c, c_sem + QUAD * back, own=not back)
    for back in range(QUAD):
        landed(back, 1, x_sem + back)
        if back >= 2:
            send(back, 1, peer_y, far_sem + back)
        send(back, 1, peer_c, c_sem + QUAD * back + 1)
        landed(back, 2, y_sem + back)
        if back < 2:
            send(back, 2, peer_x, far_sem + back)
        send(back, 2, peer_c, c_sem + QUAD * back + 2)
    for back in range(QUAD):
        landed(back, 3, far_sem + back)
        send(back, 3, peer_c, c_sem + QUAD * back + 3)
    local = [pltpu.make_async_copy(src, out.at[slot(0, 0, c_me)], local_sems.at[kind]) for kind, (src, out) in enumerate(pairs)]
    for copy in local:
        copy.start()
    for back in range(QUAD):
        for rel in range(QUAD):
            landed(back, rel, c_sem + QUAD * back + rel, 1 - c_me)
    for copy in local:
        copy.wait()
    for copy in started:
        copy.wait_send()


def gather_weights(att_block, small):
    any_spec = pl.BlockSpec(memory_space=pl.ANY)
    blocks = (att_block, small)
    return pl.pallas_call(
        weight_kernel, in_specs=[any_spec] * 2, out_specs=[any_spec] * 2,
        out_shape=[jax.ShapeDtypeStruct((32,) + block.shape, block.dtype) for block in blocks],
        scratch_shapes=[pltpu.SemaphoreType.DMA((2,)), pltpu.SemaphoreType.DMA((2, 32)), pltpu.SemaphoreType.DMA((2, 32))],
        compiler_params=pltpu.CompilerParams(collective_id=0, has_side_effects=True),
        cost_estimate=kernel_cost(att_block.size * 10 ** 5, att_block.size),
    )(*blocks)


def expert_halves(w1_expert, w3_expert, w2_expert):
    c_me = lax.axis_index('c')
    down = core_sorted(pick(w2_expert, c_me, 0), hop(pick(w2_expert, 1 - c_me, 0), 'c'))
    return [in_core_order(pick(w, c_me, 0), hop(pick(w, 1 - c_me, 0), 'c'), 0) for w in (w1_expert, w3_expert)], down


def dot32(lhs, rhs):
    return jnp.dot(lhs, rhs, preferred_element_type=F32)


def ffn_rows(rows_ref, dd_ref, w1_ref, w3_ref, w2_ref, w2_turned, wait_w2, act_ref, dg_ref, dl_ref, out_acc, back_acc):
    chunk = 512

    def step(idx, carry):
        at = pl.ds(pl.multiple_of(idx * chunk, chunk), chunk)
        gate, lin = dot_nn(rows_ref[at, :], w1_ref[:]), dot_nn(rows_ref[at, :], w3_ref[:])
        sig = jax.nn.sigmoid(gate)
        silu = gate * sig
        act = (silu * lin).astype(BF16)
        act_ref[at, :] = act
        if wait_w2 is not None:
            wait_w2(idx)
        w2 = w2_ref[:]
        d_act = (dot_nn(dd_ref[at, :], w2) if w2_turned else dot_nt(dd_ref[at, :], w2)).astype(BF16).astype(F32)
        d_lin = (d_act * silu).astype(BF16)
        d_gate = (d_act * lin * (sig + silu * (1.0 - sig))).astype(BF16)
        dg_ref[at, :] = d_gate
        dl_ref[at, :] = d_lin
        out_acc[at, :] += dot_nt(act, w2) if w2_turned else dot_nn(act, w2)
        back_acc[at, :] += dot_nt(d_gate, w1_ref[:]) + dot_nt(d_lin, w3_ref[:])
        return carry

    lax.fori_loop(0, rows_ref.shape[0] // chunk, step, 0)


def row_grads(lhs_s, grad, away, near, x_first):
    for slot in range(2):
        away[slot] = dot_nn(lhs_s[2 * slot + 1 if x_first else slot + 2], grad[:])
        near[slot] = dot_nn(lhs_s[2 * slot if x_first else slot], grad[:])


def expert_kernel(half, info, rows_ref, dd_ref, rows_t_ref, dd_t_ref, *refs):
    up_refs, down_refs, refs = refs[:8], refs[8:16], refs[16:]
    if half == 1:
        acc_in, refs = refs[:2], refs[2:]
    out_ref, back_ref, g1_away, g1_near, g3_away, g3_near, g2_away, g2_near = refs[:8]
    w1, w3, w2, act_s, dg_s, dl_s, out_acc, back_acc, lhs_s, sems = refs[8:]
    step, me = pl.program_id(0), info[0]
    same_y = (me // 2) == half
    pieces = [down_refs[2 * rel:2 * rel + 2] for rel in range(QUAD)]
    w2_halves = [w2.at[pl.ds(part * 384, 384)] for part in range(2)]
    for rel, srcs in enumerate(pieces):
        @pl.when(jnp.logical_and(same_y == (rel < 2), (step == 0) == (rel % 2 == 1)))
        def _(srcs=srcs):
            for part, src in enumerate(srcs):
                pltpu.make_async_copy(src, w2_halves[part], sems.at[part]).start()

    @pl.when(step == 0)
    def _():
        if half == 1:
            out_acc[:] = acc_in[0][:]
            back_acc[:] = acc_in[1][:]
        else:
            out_acc[:] = jnp.zeros_like(out_acc)
            back_acc[:] = jnp.zeros_like(back_acc)
        for rel in range(QUAD):
            lhs_s[rel] = rows_t_ref[pl.ds(pl.multiple_of((me ^ rel) * 192, 64), 192), :]

    for rel in range(QUAD):
        at = pl.ds(pl.multiple_of((me ^ rel) * 192, 64), 192)
        w1[at, :], w3[at, :] = (ref[:] for ref in up_refs[2 * rel:2 * rel + 2])

    def wait_w2(idx):
        @pl.when(idx == 0)
        def _():
            for part, src in enumerate(pieces[0]):
                pltpu.make_async_copy(src, w2_halves[part], sems.at[part]).wait()

    ffn_rows(rows_ref, dd_ref, w1, w3, w2, False, wait_w2, act_s, dg_s, dl_s, out_acc, back_acc)
    row_grads(lhs_s, dg_s, g1_away, g1_near, True)
    row_grads(lhs_s, dl_s, g3_away, g3_near, False)

    for near in range(2):
        @pl.when(step == near)
        def _(g2_ref=(g2_away, g2_near)[near]):
            for part in range(2):
                at = slice(part * 384, part * 384 + 384)
                g2_ref[at, :] = dot_nn(dd_t_ref[at, :], act_s[:])

    @pl.when(step == 1)
    def _():
        out_ref[:] = out_acc[:].astype(out_ref.dtype)
        back_ref[:] = back_acc[:].astype(back_ref.dtype)


def expert_half(half, rows, dd, rows_t, dd_t, up, down, acc):
    tok, dim = rows.shape
    y_me, x_me = lax.axis_index('y'), lax.axis_index('x')
    info = jnp.stack([2 * y_me + x_me, 2 * half + 1 - x_me, 2 * half + x_me]).astype(jnp.int32)
    whole, turned = fixed(tok, dim), fixed(dim, tok)

    up_spec = pl.BlockSpec((dim // QUAD, dim), lambda step, info_ref: (0, info_ref[1 + step]))
    any_spec = pl.BlockSpec(memory_space=pl.ANY)
    row_out = pl.BlockSpec((2, dim // QUAD, dim), lambda step, info_ref: (0, 0, info_ref[1 + step] - 2 * half))
    square = fixed(dim, dim)
    acc_type = F32 if half == 0 else BF16
    row_shape, square_shape = jax.ShapeDtypeStruct((2, dim // QUAD, 2 * dim), F32), jax.ShapeDtypeStruct((dim, dim), F32)
    return pl.pallas_call(
        lambda *refs: expert_kernel(half, *refs),
        grid_spec=pltpu.PrefetchScalarGridSpec(
            num_scalar_prefetch=1, grid=(2,),
            in_specs=[whole, whole, turned, turned] + [up_spec] * 8 + [any_spec] * 8 + [whole] * len(acc),
            out_specs=[whole, whole] + [row_out] * QUAD + [square] * 2,
            scratch_shapes=[pltpu.VMEM((dim, dim), BF16)] * 3 + [pltpu.VMEM((tok, dim), BF16)] * 3 + [pltpu.VMEM((tok, dim), F32)] * 2 + [pltpu.VMEM((QUAD, dim // QUAD, tok), BF16), pltpu.SemaphoreType.DMA((2,))]),
        out_shape=[jax.ShapeDtypeStruct((tok, dim), acc_type)] * 2 + [row_shape] * QUAD + [square_shape] * 2,
        compiler_params=pltpu.CompilerParams(vmem_limit_bytes=VMEM_LIMIT),
        cost_estimate=kernel_cost(36 * tok * dim * dim, dim * dim),
    )(info, rows, dd, rows_t, dd_t, *up, *down, *acc)


def shared_kernel(info, rows_ref, dd_ref, rows_t_ref, dd_t_ref, *refs):
    pieces, refs = [refs[8 * mat:8 * mat + 8] for mat in range(3)], refs[24:]
    out_refs, back_refs, g3_away, g3_near, g1_refs, g2_refs = refs[:2], refs[2:4], refs[4], refs[5], refs[6:10], refs[10:14]
    w1, w3, w2, act_s, dg_s, dl_s, out_acc, back_acc, lhs_s, lhs_z, dd_z = refs[14:]
    step, me, z_me = pl.program_id(0), info[0], info[1]

    def spot(rel, turn_z):
        return pl.ds(pl.multiple_of(((z_me ^ turn_z) * QUAD + (me ^ rel)) * ROWS, 16), ROWS)

    @pl.when(step == 0)
    def _():
        out_acc[:] = jnp.zeros_like(out_acc)
        back_acc[:] = jnp.zeros_like(back_acc)
        for rel in range(QUAD):
            for turn_z in range(QUAD):
                inner = slice(rel * ROWS, rel * ROWS + ROWS)
                lhs_s[rel, turn_z * ROWS:turn_z * ROWS + ROWS, :] = rows_t_ref[spot(rel, turn_z), :]
                lhs_z[turn_z, inner, :] = rows_t_ref[spot(rel, turn_z), :]
                dd_z[turn_z, inner, :] = dd_t_ref[spot(rel, turn_z), :]

    for w_ref, halves in zip((w1, w3, w2), pieces):
        for turn_z in range(QUAD):
            for rel in range(QUAD):
                w_ref[spot(rel, turn_z), :] = halves[2 * rel + turn_z // 2][turn_z % 2]

    ffn_rows(rows_ref, dd_ref, w1, w3, w2, True, None, act_s, dg_s, dl_s, out_acc, back_acc)
    row_grads(lhs_s, dl_s, g3_away, g3_near, True)
    for turn_z in range(QUAD):
        g1_refs[turn_z][:] = dot_nn(lhs_z[turn_z], dg_s[:])
        g2_refs[turn_z][:] = dot_nn(dd_z[turn_z], act_s[:])

    @pl.when(step == pl.num_programs(0) - 1)
    def _():
        for acc, halves in ((out_acc, out_refs), (back_acc, back_refs)):
            for ref, value in zip(halves, jnp.split(acc[:], 2, axis=0)):
                ref[:] = value


def shared_ffn(gate, rows, dd, rows_t, dd_t, pieces):
    tok, dim = rows.shape
    width = pieces[0].shape[2] // 3
    steps = width // dim
    info = after(jnp.stack([2 * lax.axis_index('y') + lax.axis_index('x'), lax.axis_index('z')]).astype(jnp.int32), gate)
    whole, turned, half = fixed(tok, dim), fixed(dim, tok), fixed(tok // 2, dim)
    piece_specs = [pl.BlockSpec((2, ROWS, dim), lambda step, info_ref, mat=mat: (0, 0, mat * steps + step)) for mat in range(3) for _ in pieces]
    row_out = pl.BlockSpec((2, dim // QUAD, dim), lambda step, info_ref: (0, 0, step))
    z_out = pl.BlockSpec((dim // QUAD, dim), lambda step, info_ref: (0, step))
    shapes = ((tok // 2, dim),) * QUAD + ((2, dim // QUAD, width),) * 2 + ((dim // QUAD, width),) * 8
    outs = pl.pallas_call(
        shared_kernel,
        grid_spec=pltpu.PrefetchScalarGridSpec(
            num_scalar_prefetch=1, grid=(steps,),
            in_specs=[whole, whole, turned, turned] + piece_specs,
            out_specs=[half] * QUAD + [row_out] * 2 + [z_out] * 8,
            scratch_shapes=[pltpu.VMEM((dim, dim), BF16)] * 3 + [pltpu.VMEM((tok, dim), BF16)] * 3 + [pltpu.VMEM((tok, dim), F32)] * 2 + [pltpu.VMEM((QUAD, dim // QUAD, tok), BF16)] * 3),
        out_shape=[jax.ShapeDtypeStruct(shape, F32) for shape in shapes],
        compiler_params=pltpu.CompilerParams(vmem_limit_bytes=VMEM_LIMIT),
        cost_estimate=kernel_cost(18 * tok * dim * width, dim * width),
    )(info, rows, dd, rows_t, dd_t, *(list(pieces) * 3))
    return outs[:2], outs[2:4], outs[4:6], outs[6:10], outs[10:]


def z_sum(plane):
    summed = plane[0]
    for step in (1, 2, 3):
        summed = summed + z_hop(plane[step], step)
    return summed


def swap_rows(summed):
    halves = summed.reshape(summed.shape[:-2] + (2, -1, summed.shape[-1]))
    axis, c_me = halves.ndim - 3, lax.axis_index('c')
    return pick(halves, c_me, axis), hop(pick(halves, 1 - c_me, axis), 'c')


def plane_sum_values(total):
    y_me, x_me = lax.axis_index('y'), lax.axis_index('x')
    ways = tuple(zip((total[:2], total[2:]), ((2, x_me, y_me, 'x', 'y'), (1, y_me, x_me, 'y', 'x'))))
    gives = [pick(part, 1 - me_1, axis_1) for part, (axis_1, me_1, *_) in ways]

    def rest():
        planes = []
        for give, (part, (axis_1, me_1, me_2, name_1, name_2)) in zip(gives, ways):
            got, keep = hop(give, name_1), pick(part, me_1, axis_1)
            got_2 = hop(pick(keep, 1 - me_2, 1) + pick(got, 1 - me_2, 1), name_2)
            planes.append(pick(keep, me_2, 1) + pick(got, me_2, 1) + got_2)
        return jnp.concatenate(planes, axis=0)

    return gives, rest


def layer_step(x_in, grad_y, w_q, w_k, w_v, w_o, gamma_attn, gamma_mlp, w_router, w1_shared, w3_shared, w2_shared, w1_expert, w3_expert, w2_expert, expert_ids):
    n_batch, seq_len, model_dim = x_in.shape
    n_tok = n_batch * seq_len
    n_heads, head_dim = w_q.shape[1], w_q.shape[2]
    att_dim, att_half = n_heads * head_dim, n_heads * head_dim // 2
    n_experts = w_router.shape[1]
    ff_half = w1_shared.shape[1] // 2
    capacity = 2 * n_tok // n_experts
    n_slots = n_experts * capacity

    up_own, down_own = expert_halves(w1_expert, w3_expert, w2_expert)
    down_x, down_y = plane_near(down_own)
    w_q, w_k, w_v, w_o = (after(weight, *down_own) for weight in (w_q, w_k, w_v, w_o))
    att_parts = (w_q.reshape(-1, att_dim), w_k.reshape(-1, att_dim), w_v.reshape(-1, att_dim), w_o.reshape(att_dim, -1).T)
    att_block = jnp.concatenate([part[:, :att_half] for part in att_parts] + [part[:, att_half:] for part in att_parts], axis=1)
    small = jnp.concatenate([gamma_attn.astype(F32)[:, None], gamma_mlp.astype(F32)[:, None], w_router], axis=1)
    small = jnp.pad(small, ((0, 0), (0, LANES - small.shape[1])))
    att_all, small_all = gather_weights(att_block, small)
    att_all, small_all = att_all.reshape(model_dim, -1), small_all.reshape(model_dim, -1)
    ga_all, gm_all, wr_all = small_all[:, 0], small_all[:, 1], small_all[:, 2:2 + n_experts]

    def far(from_x, from_y, *gates):
        return [hop(after(from_y[0], *gates), 'x'), hop(after(from_x[1], *gates), 'y')]

    down_far = far(down_x, down_y, small_all)
    up_x, up_y = plane_near(up_own)
    sh_parts = z_parts([after(weight, small_all) for weight in (w1_shared, w3_shared, w2_shared.T)])

    d_out = grad_y.reshape(n_tok, model_dim)
    onehot, dest_row = route_slots(expert_ids.reshape(n_tok), n_experts, capacity)
    place = (dest_row[:, None] == jnp.arange(n_slots)[None, :]).astype(BF16)

    def exchange(values):
        return lax.all_to_all(values.reshape(n_experts, capacity, model_dim), ('z', 'c'), 0, 0, tiled=True).reshape(n_slots, model_dim)

    def dispatch(values):
        return jnp.einsum('ts,td->sd', place, values, preferred_element_type=F32).astype(BF16)

    d_out_both = jnp.concatenate([d_out, hop(d_out, 'c')], axis=0)
    d_out_t = d_out_both.T
    tables = rope_tables(seq_len, head_dim)

    tokens = x_in.reshape(n_tok, model_dim)
    qkv, normed1 = norm_qkv(tokens, ga_all[None, :], att_all)
    norm1_pull = jax.vjp(rms_norm, tokens, ga_all)[1]
    heads = attn_call(attn_fwd_kernel, 8, qkv, None, *tables, pair_spec(n_tok), att_dim)
    half_cols = [slice(start, start + att_half) for start in (0, att_half)]
    wot = [att_all[:, start + 3 * att_half:start + QUAD * att_half] for start in (0, QUAD * att_half)]
    attn_out = sum(jnp.einsum('tk,dk->td', heads[:, cols], w_half, preferred_element_type=F32) for cols, w_half in zip(half_cols, wot))
    hidden = (tokens.astype(F32) + attn_out).astype(BF16)
    normed2, norm2_pull = jax.vjp(rms_norm, hidden, gm_all)
    normed2_f = normed2.astype(F32)
    logits = jnp.dot(normed2, wr_all, preferred_element_type=F32, precision=lax.Precision.HIGHEST)
    gate_val = jax.nn.sigmoid(jnp.sum(jnp.where(onehot, logits, 0.0), axis=1))
    routed_in = (gate_val[:, None] * normed2_f).astype(BF16)
    give_r = dispatch(routed_in)
    give_d = dispatch(after(d_out, give_r))
    rows = exchange(give_r)
    d_down = exchange(after(give_d, rows))
    rows_t, d_down_t = rows.T, d_down.T

    normed2_both = jnp.concatenate([normed2, hop(normed2, 'c')], axis=0)
    normed2_t = normed2_both.T
    sh_parts = [after(part, heads) for part in sh_parts]
    sh_own = jnp.stack(sh_parts[:2]), jnp.stack(sh_parts[2:])
    sh_x, sh_y = plane_near(sh_own)

    up_far = far(up_x, up_y, give_r)
    sh_far = far(sh_x, sh_y, give_r, give_d, normed2_t, d_out_t)
    sh_pieces, up_pieces, down_pieces = ([*own, *from_x, *from_y, *diag] for own, from_x, from_y, diag in ((sh_own, sh_x, sh_y, sh_far), (up_own, up_x, up_y, up_far), (down_own, down_x, down_y, down_far)))
    shared_part, d_part, (s3_away, s3_near), s1, s2 = shared_ffn(rows_t, normed2_both, d_out_both, normed2_t, d_out_t, sh_pieces)
    shared_out = shared_part[0] + hop(shared_part[1], 'c')
    d_normed2 = d_part[0] + hop(d_part[1], 'c')

    *acc, a1_away, a1_near, a3_away, a3_near, a2_away, a2_near = expert_half(0, rows, d_down, rows_t, d_down_t, up_pieces, down_pieces, ())
    down_rows, d_rows, b1_away, b1_near, b3_away, b3_near, b2_away, b2_near = expert_half(1, rows, d_down, rows_t, d_down_t, up_pieces, down_pieces, acc)
    d_back = exchange(d_rows)

    def first_sum(away, near, axis, gate):
        keep, give = near + after(hop(away, axis), *gate)
        return keep, hop(give, 'y' if axis == 'x' else 'x')

    s3 = first_sum(s3_away, s3_near, 'x', [d_rows])
    a1 = first_sum(a1_away, a1_near, 'x', [d_rows])
    d_routed_in = jnp.einsum('ts,sd->td', place, d_back, preferred_element_type=F32)
    d_normed2 = d_normed2 + gate_val[:, None] * d_routed_in
    d_gate_val = jnp.sum(d_routed_in * normed2_f, axis=1) * gate_val * (1.0 - gate_val)
    d_logits = jnp.where(onehot, d_gate_val[:, None], 0.0)
    g_wr = jnp.einsum('td,te->de', normed2_f, d_logits, precision=lax.Precision.HIGHEST)
    d_normed2 = d_normed2 + jnp.einsum('te,de->td', d_logits, wr_all, precision=lax.Precision.HIGHEST)
    d_hid_norm, g_gm = norm2_pull(d_normed2.astype(BF16))
    d_hidden = (d_out.astype(F32) + d_hid_norm.astype(F32)).astype(BF16)

    d_hidden_t, normed1_t = d_hidden.T, normed1.T
    d_heads = jnp.concatenate([dot32(d_hidden, w_half).astype(BF16) for w_half in wot], axis=1)
    d_qkv = attn_call(attn_bwd_kernel, 16, qkv, d_heads, *tables, fixed(n_tok, 3 * att_dim), 3 * att_dim)
    d_halves = jnp.split(d_qkv, 2, axis=1)
    d_normed1 = sum(jnp.einsum('tk,dk->td', half, att_all[:, start:start + 3 * att_half], preferred_element_type=F32) for half, start in zip(d_halves, (0, QUAD * att_half)))
    d_tok_norm, g_ga = norm1_pull(d_normed1.astype(BF16))
    g_small = jnp.concatenate([g_ga[:, None], g_gm[:, None], g_wr, jnp.zeros((model_dim, 6), F32)], axis=1)
    core_0 = lax.axis_index('c') == 0

    def core_pick(pair):
        first, second = pair
        return jnp.where(core_0, first, second), jnp.where(core_0, second, first)

    g_att = []
    for lhs_t, pair in ((normed1_t, d_halves), (d_hidden_t, [heads[:, cols] for cols in half_cols])):
        mine, other = core_pick(pair)
        g_att.append(dot32(lhs_t, mine) + hop(dot32(lhs_t, other), 'c'))
    mine, other = (jnp.pad(half, ((0, 0), (0, LANES - half.shape[1]))) for half in core_pick(jnp.split(g_small, 2, axis=1)))
    g_att.append(mine + hop(other, 'c'))
    att_gives, att_rest = plane_sum_values(jnp.concatenate(g_att, axis=1).reshape(QUAD, 2, 2, ROWS, -1))

    def later(value):
        return after(value, *att_gives)

    low_y = lax.axis_index('y') == 0
    g2_low, g2_high = a2_near + later(hop(a2_away, 'x')), b2_near + later(hop(b2_away, 'x'))
    g2_keep, g2_give = jnp.where(low_y, g2_low, g2_high), jnp.where(low_y, g2_high, g2_low)

    def z_first(parts):
        total = parts[0]
        for step in Z_STEPS:
            total = total + after(z_hop(parts[step], step), g2_give)
        return jnp.split(total.reshape(2, 2, ROWS, -1), 2, axis=1)

    def z_last(pair):
        keep, give = pair
        keep, give = keep + hop(give, 'x')
        return (keep + hop(give, 'y')).reshape(ROWS, -1)

    s1, s2 = z_first(s1), z_first(s2)
    b_gates = [s1[1], s2[1]]
    routed = jnp.einsum('ts,sd->td', place, exchange(later(down_rows)), preferred_element_type=F32)
    layer_out = (hidden.astype(F32) + routed + shared_out).astype(BF16)
    a3 = first_sum(a3_away, a3_near, 'y', att_gives)
    b1, b3 = first_sum(b1_away, b1_near, 'x', b_gates), first_sum(b3_away, b3_near, 'y', b_gates)

    def finish(pair, *gates):
        mine, got = pair
        return mine + later(after(got, *gates) if gates else got)

    def rows_by_expert(pairs, *gates):
        return in_core_order(*(part[None] for part in swap_rows(jnp.stack([finish(pair, *gates) for pair in pairs]))), 0)

    g_up = jnp.concatenate([rows_by_expert((a1, a3), b1[0], b3[0]), rows_by_expert((b1, b3))], axis=-1)
    g2_mine, g2_other = core_halves(g2_keep + hop(g2_give, 'y'), 1)
    g_w2e = in_core_order(g2_mine.T[None], hop(g2_other, 'c').T[None], 0)
    g_sh = jnp.concatenate([z_last(s1), z_sum(finish(s3).reshape(QUAD, ROWS, -1)), z_last(s2)], axis=1)
    g_sh_mine, g_sh_other = swap_rows(g_sh)
    z_me = lax.axis_index('z')
    att_plane = att_rest()
    g_att_mine, g_att_other = swap_rows(z_sum([pick(att_plane, z_me ^ step, 0) for step in range(QUAD)]))
    d_x = (d_hidden.astype(F32) + d_tok_norm.astype(F32)).astype(BF16).reshape(n_batch, seq_len, model_dim)

    g_small = in_core_order(*(part[:, QUAD * att_half:QUAD * att_half + 8] for part in (g_att_mine, g_att_other)), 1)
    g_att_mine, g_att_other = g_att_mine[:, :QUAD * att_half], g_att_other[:, :QUAD * att_half]
    g_att = in_core_order(g_att_mine.reshape(-1, QUAD, att_half), g_att_other.reshape(-1, QUAD, att_half), 2)
    g_q, g_k, g_v = (g_att[:, part].reshape(-1, n_heads, head_dim) for part in range(3))
    g_wo = g_att[:, 3].T.reshape(n_heads, head_dim, -1)
    g_sh = in_core_order(g_sh_mine.reshape(-1, 3, ff_half), g_sh_other.reshape(-1, 3, ff_half), 2)
    return (layer_out.reshape(n_batch, seq_len, model_dim), d_x, g_q, g_k, g_v, g_wo, g_small[:, 0], g_small[:, 1], g_small[:, 2:2 + n_experts], g_sh[:, 0], g_sh[:, 1], g_sh[:, 2].T, g_up[:, 0], g_up[:, 1], g_w2e)


def solution(mesh):
    fine_mesh = Mesh(np.asarray(mesh.devices).reshape(4, 2, 2, 2), AXES)
    row_spec, wo_spec, w2s_spec, exp_spec = P(AXES), P(None, None, AXES), P(None, AXES), P('z', AXES[1:])
    weight_specs = (row_spec,) * 3 + (wo_spec,) + (row_spec,) * 5 + (w2s_spec,) + (exp_spec,) * 3
    out_specs = (row_spec, row_spec) + weight_specs
    in_specs = out_specs + (row_spec,)
    return jax.shard_map(layer_step, mesh=fine_mesh, in_specs=in_specs, out_specs=out_specs, check_vma=False)
```

```python
import jax
import jax.numpy as jnp
import numpy as np
from jax import lax
from jax.experimental import pallas as pl
from jax.experimental.pallas import tpu as pltpu
from jax.sharding import Mesh, PartitionSpec as P

LANES = 128
ROWS = 48
QUAD = 4
EPS_NORM = 1e-5
EPS_QK = 1e-6
ROPE_BASE = 500000.0
QUERY_BLOCK = 256
VMEM_LIMIT = 60 * 1024 * 1024
AXES = ('z', 'y', 'x', 'c')
Z_STEPS = (1, 2, 3)
SWAP = ((0, 1), (1, 0))
F32 = jnp.float32
BF16 = jnp.bfloat16


def rms_norm(tokens, gamma_vec):
    tok_f32 = tokens.astype(F32)
    inv_rms = lax.rsqrt(jnp.mean(tok_f32 * tok_f32, axis=-1, keepdims=True) + EPS_NORM)
    return (tok_f32 * inv_rms * gamma_vec.astype(F32)).astype(BF16)


def rope_tables(seq_len, head_dim):
    half_dim = head_dim // 2
    steps = np.arange(half_dim, dtype=np.float32) * np.float32(2.0 / head_dim)
    inv_freq = np.power(np.float32(ROPE_BASE), -steps)
    angles = np.arange(seq_len, dtype=np.float32)[:, None] * inv_freq[None, :]
    cos_tab, sin_tab = np.cos(angles), np.sin(angles)
    return jnp.asarray(np.tile(cos_tab, (1, 4))), jnp.asarray(np.tile(np.concatenate([-sin_tab, sin_tab], axis=1), (1, 2)))


def lane_masks(rows):
    lane = lax.broadcasted_iota(jnp.int32, (rows, LANES), 1)
    return lane % 64 < 32, lane < 64


def turn(vals, cos_tab, sin_tab, low_half):
    partner = jnp.where(low_half, pltpu.roll(vals, 96, 1), pltpu.roll(vals, 32, 1))
    return vals * cos_tab + partner * sin_tab


def head_mean(vals, head_a):
    sum_a = jnp.sum(jnp.where(head_a, vals, 0.0), axis=1, keepdims=True)
    sum_b = jnp.sum(jnp.where(head_a, 0.0, vals), axis=1, keepdims=True)
    return jnp.where(head_a, sum_a, sum_b) * (1.0 / 64)


def rope_norm(vals, cos_tab, sin_tab, low_half, head_a):
    rotated = turn(vals.astype(F32), cos_tab, sin_tab, low_half)
    inv = lax.rsqrt(head_mean(rotated * rotated, head_a) + EPS_QK)
    return rotated, inv, (rotated * inv).astype(BF16)


def rope_norm_back(d_out, rotated, inv, cos_tab, sin_tab, low_half, head_a):
    d_rot = inv * d_out - rotated * (inv * inv * inv * head_mean(d_out * rotated, head_a))
    return turn(d_rot, cos_tab, -sin_tab, low_half).astype(BF16)


def dot_nn(lhs, rhs):
    return jnp.einsum('ik,kj->ij', lhs, rhs, preferred_element_type=F32)


def dot_nt(lhs, rhs):
    return jnp.einsum('ik,jk->ij', lhs, rhs, preferred_element_type=F32)


def dot_tn(lhs, rhs):
    return jnp.einsum('ki,kj->ij', lhs, rhs, preferred_element_type=F32)


def softmax_block(q_rows, k_all, start, keys):
    scores = dot_nt(q_rows, k_all[:keys]) * 0.125
    row = start + lax.broadcasted_iota(jnp.int32, scores.shape, 0)
    col = lax.broadcasted_iota(jnp.int32, scores.shape, 1)
    scores = jnp.where(row >= col, scores, -1e30)
    weights = jnp.exp(scores - jnp.max(scores, axis=1, keepdims=True))
    return weights / jnp.sum(weights, axis=1, keepdims=True)


def attn_fwd_kernel(q_ref, k_ref, v_ref, cos_ref, sin_ref, o_ref):
    seq = q_ref.shape[0]
    low_half, head_a = lane_masks(seq)
    cos_tab, sin_tab = cos_ref[:], sin_ref[:]
    q_rot = rope_norm(q_ref[:], cos_tab, sin_tab, low_half, head_a)[-1]
    k_rot = rope_norm(k_ref[:], cos_tab, sin_tab, low_half, head_a)[-1]
    v_all = v_ref[:]
    zero = jnp.zeros_like(q_rot)
    q_heads = jnp.where(head_a, q_rot, zero), jnp.where(head_a, zero, q_rot)
    for start in range(0, seq, QUERY_BLOCK):
        keys = start + QUERY_BLOCK
        outs = [dot_nn(softmax_block(q_head[start:keys], k_rot, start, keys).astype(BF16), v_all[:keys]) for q_head in q_heads]
        o_ref[start:keys, :] = jnp.where(head_a[:QUERY_BLOCK], outs[0], outs[1]).astype(BF16)


def attn_bwd_kernel(q_ref, k_ref, v_ref, do_ref, cos_ref, sin_ref, d_ref):
    seq = q_ref.shape[0]
    low_half, head_a = lane_masks(seq)
    cos_tab, sin_tab = cos_ref[:], sin_ref[:]
    q_raw, q_inv, q_rot = rope_norm(q_ref[:], cos_tab, sin_tab, low_half, head_a)
    k_raw, k_inv, k_rot = rope_norm(k_ref[:], cos_tab, sin_tab, low_half, head_a)
    v_all, d_o = v_ref[:], do_ref[:]
    zero = jnp.zeros_like(q_rot)
    grads = []
    for head in range(2):
        def only(vals, head=head):
            return jnp.where(head_a, vals, zero) if head == 0 else jnp.where(head_a, zero, vals)

        q_head, do_head = only(q_rot), only(d_o)
        dq_rows, dk_sum, dv_sum = [], None, None
        for start in range(0, seq, QUERY_BLOCK):
            keys = start + QUERY_BLOCK
            probs = softmax_block(q_head[start:keys], k_rot, start, keys)
            d_probs = dot_nt(do_head[start:keys], v_all[:keys])
            d_scores = probs * (d_probs - jnp.sum(probs * d_probs, axis=1, keepdims=True)) * 0.125
            d_scores = d_scores.astype(BF16)
            dq_rows.append(dot_nn(d_scores, k_rot[:keys]))
            dk_part = dot_tn(d_scores, q_head[start:keys])
            dv_part = dot_tn(probs.astype(BF16), do_head[start:keys])
            if keys < seq:
                pad = jnp.zeros((seq - keys, LANES), F32)
                dk_part, dv_part = jnp.concatenate([dk_part, pad]), jnp.concatenate([dv_part, pad])
            dk_sum = dk_part if dk_sum is None else dk_sum + dk_part
            dv_sum = dv_part if dv_sum is None else dv_sum + dv_part
        grads.append((jnp.concatenate(dq_rows), dk_sum, dv_sum))
    d_q, d_k, d_v = (jnp.where(head_a, part_a, part_b) for part_a, part_b in zip(*grads))
    rotary = (cos_tab, sin_tab, low_half, head_a)
    parts = rope_norm_back(d_q, q_raw, q_inv, *rotary), rope_norm_back(d_k, k_raw, k_inv, *rotary), d_v.astype(BF16)
    for part, value in enumerate(parts):
        block = column_block(pl.program_id(0), part)
        d_ref[:, pl.ds(pl.multiple_of(block * LANES, LANES), LANES)] = value


def column_block(pair, part):
    return pair // 3 * 9 + part * 3 + pair % 3


def qkv_kernel(x_ref, gamma_ref, w_ref, qkv_ref, n_ref):
    @pl.when(pl.program_id(0) == 0)
    def _():
        n_ref[:] = rms_norm(x_ref[:], gamma_ref[:])

    qkv_ref[:] = dot_nn(n_ref[:], w_ref[:]).astype(BF16)


def norm_qkv(tokens, gamma, weights):
    (tok, dim), width = tokens.shape, weights.shape[1] // 8
    return pl.pallas_call(
        qkv_kernel, grid=(6,), in_specs=[fixed(tok, dim), fixed(1, dim), pl.BlockSpec((dim, width), lambda step: (0, step + step // 3))],
        out_specs=[pl.BlockSpec((tok, width), lambda step: (0, step)), fixed(tok, dim)],
        out_shape=[jax.ShapeDtypeStruct((tok, 6 * width), BF16), jax.ShapeDtypeStruct((tok, dim), BF16)],
        compiler_params=pltpu.CompilerParams(vmem_limit_bytes=VMEM_LIMIT),
        cost_estimate=kernel_cost(12 * tok * dim * width, dim * width),
    )(tokens, gamma, weights)


def fixed(*shape):
    return pl.BlockSpec(shape, lambda *_: (0,) * len(shape))


def kernel_cost(flops, moved):
    return pl.CostEstimate(flops=flops, bytes_accessed=moved, transcendentals=0)


def attn_call(kernel, name_cost, qkv, d_o, cos_tab, sin_tab, out_spec, out_width):
    seq = qkv.shape[0]
    head_specs = [pl.BlockSpec((seq, LANES), lambda pair, part=part: (0, column_block(pair, part))) for part in range(3)]
    table = fixed(seq, LANES)
    extra = [] if d_o is None else [pair_spec(seq)]
    return pl.pallas_call(
        kernel, grid=(6,), in_specs=head_specs + extra + [table, table], out_specs=out_spec, out_shape=jax.ShapeDtypeStruct((seq, out_width), BF16),
        compiler_params=pltpu.CompilerParams(vmem_limit_bytes=VMEM_LIMIT), cost_estimate=kernel_cost(name_cost * seq * seq * seq, qkv.size),
    )(qkv, qkv, qkv, *([] if d_o is None else [d_o]), cos_tab, sin_tab)


def pair_spec(seq):
    return pl.BlockSpec((seq, LANES), lambda pair: (0, pair))


def route_slots(flat_ids, n_experts, capacity):
    onehot = flat_ids[:, None] == jnp.arange(n_experts)[None, :]
    token = jnp.arange(flat_ids.size)
    before = (token[:, None] > token[None, :]).astype(BF16)
    running = jnp.dot(before, onehot.astype(BF16), preferred_element_type=F32)
    slot_idx = jnp.sum(jnp.where(onehot, running, 0.0), axis=1).astype(jnp.int32)
    return onehot, flat_ids * capacity + slot_idx


def hop(block, axis):
    return lax.ppermute(block, axis, SWAP)


def z_hop(block, step):
    return lax.ppermute(block, 'z', [(z_idx, z_idx ^ step) for z_idx in range(QUAD)])


def pick(array, idx, axis):
    return lax.dynamic_index_in_dim(array, idx, axis, keepdims=False)


def core_sorted(mine, other):
    first = lax.axis_index('c') == 0
    return jnp.where(first, mine, other), jnp.where(first, other, mine)


def in_core_order(mine, other, axis):
    return jnp.concatenate(core_sorted(mine, other), axis=axis)


def core_halves(array, axis):
    low, high = jnp.split(array, 2, axis=axis)
    first = lax.axis_index('c') == 0
    return jnp.where(first, low, high), jnp.where(first, high, low)


def plane_near(halves):
    return [hop(half, 'x') for half in halves], [hop(half, 'y') for half in halves]


def after(value, *anchors):
    return lax.optimization_barrier((value,) + anchors)[0]


def shared_chip(parts):
    half = parts[0].shape[1] // 2
    c_me = lax.axis_index('c')

    def side(core):
        return jnp.concatenate([lax.dynamic_slice_in_dim(part, core * half, half, axis=1) for part in parts], axis=1)

    return in_core_order(side(c_me), hop(side(1 - c_me), 'c'), 0)


def weight_kernel(att_ref, small_ref, att_out, small_out, local_sems, send_sems, recv_sems):
    z_me, y_me, x_me, c_me = (lax.axis_index(name) for name in AXES)
    peers = [((z_me + step) % 4, y_me, x_me, c_me) for step in Z_STEPS]
    peer_x, peer_y, peer_c = (z_me, y_me, 1 - x_me, c_me), (z_me, 1 - y_me, x_me, c_me), (z_me, y_me, x_me, 1 - c_me)
    barrier = pltpu.get_barrier_semaphore()
    everyone = peers + [peer_x, peer_y, peer_c]
    for peer in everyone:
        pl.semaphore_signal(barrier, inc=1, device_id=peer, device_id_type=pl.DeviceIdType.MESH)
    pl.semaphore_wait(barrier, len(everyone))

    def slot(back, rel, core):
        y_at, x_at = (1 - y_me if rel >= 2 else y_me), (1 - x_me if rel % 2 else x_me)
        return (((z_me + 4 - back) % 4 * 2 + y_at) * 2 + x_at) * 2 + core

    pairs = ((att_ref, att_out), (small_ref, small_out))

    started = []

    def send(back, rel, peer, sem, own=False):
        at = slot(back, rel, c_me)
        for kind, (src, out) in enumerate(pairs):
            copy = pltpu.make_async_remote_copy(
                src_ref=src if own else out.at[at], dst_ref=out.at[at], send_sem=send_sems.at[kind, sem], recv_sem=recv_sems.at[kind, sem],
                device_id=peer, device_id_type=pl.DeviceIdType.MESH)
            copy.start()
            started.append(copy)

    def landed(back, rel, sem, core=c_me):
        for kind, (src, out) in enumerate(pairs):
            pltpu.make_async_copy(src, out.at[slot(back, rel, core)], recv_sems.at[kind, sem]).wait()

    z_sem, x_sem, y_sem, far_sem, c_sem = range(0, 20, 4)
    for step, peer in zip(Z_STEPS, peers):
        send(0, 0, peer, z_sem + step, own=True)
    for back in range(QUAD):
        if back:
            landed(back, 0, z_sem + back)
        send(back, 0, peer_x, x_sem + back, own=not back)
        send(back, 0, peer_y, y_sem + back, own=not back)
        send(back, 0, peer_c, c_sem + QUAD * back, own=not back)
    for back in range(QUAD):
        landed(back, 1, x_sem + back)
        if back >= 2:
            send(back, 1, peer_y, far_sem + back)
        send(back, 1, peer_c, c_sem + QUAD * back + 1)
        landed(back, 2, y_sem + back)
        if back < 2:
            send(back, 2, peer_x, far_sem + back)
        send(back, 2, peer_c, c_sem + QUAD * back + 2)
    for back in range(QUAD):
        landed(back, 3, far_sem + back)
        send(back, 3, peer_c, c_sem + QUAD * back + 3)
    local = [pltpu.make_async_copy(src, out.at[slot(0, 0, c_me)], local_sems.at[kind]) for kind, (src, out) in enumerate(pairs)]
    for copy in local:
        copy.start()
    for back in range(QUAD):
        for rel in range(QUAD):
            landed(back, rel, c_sem + QUAD * back + rel, 1 - c_me)
    for copy in local:
        copy.wait()
    for copy in started:
        copy.wait_send()


def gather_weights(att_block, small):
    any_spec = pl.BlockSpec(memory_space=pl.ANY)
    blocks = (att_block, small)
    return pl.pallas_call(
        weight_kernel, in_specs=[any_spec] * 2, out_specs=[any_spec] * 2,
        out_shape=[jax.ShapeDtypeStruct((32,) + block.shape, block.dtype) for block in blocks],
        scratch_shapes=[pltpu.SemaphoreType.DMA((2,)), pltpu.SemaphoreType.DMA((2, 32)), pltpu.SemaphoreType.DMA((2, 32))],
        compiler_params=pltpu.CompilerParams(collective_id=0, has_side_effects=True),
        cost_estimate=kernel_cost(att_block.size * 10 ** 5, att_block.size),
    )(*blocks)


def expert_halves(w1_expert, w3_expert, w2_expert):
    c_me = lax.axis_index('c')
    down = core_sorted(pick(w2_expert, c_me, 0), hop(pick(w2_expert, 1 - c_me, 0), 'c'))
    return [in_core_order(pick(w, c_me, 0), hop(pick(w, 1 - c_me, 0), 'c'), 0) for w in (w1_expert, w3_expert)], down


def dot32(lhs, rhs):
    return jnp.dot(lhs, rhs, preferred_element_type=F32)


def ffn_rows(rows_ref, dd_ref, w1_ref, w3_ref, w2_ref, w2_turned, wait_w2, act_ref, dg_ref, dl_ref, out_acc, back_acc):
    chunk = 512

    def step(idx, carry):
        at = pl.ds(pl.multiple_of(idx * chunk, chunk), chunk)
        gate, lin = dot_nn(rows_ref[at, :], w1_ref[:]), dot_nn(rows_ref[at, :], w3_ref[:])
        sig = jax.nn.sigmoid(gate)
        silu = gate * sig
        act = (silu * lin).astype(BF16)
        act_ref[at, :] = act
        if wait_w2 is not None:
            wait_w2(idx)
        w2 = w2_ref[:]
        d_act = (dot_nn(dd_ref[at, :], w2) if w2_turned else dot_nt(dd_ref[at, :], w2)).astype(BF16).astype(F32)
        d_lin = (d_act * silu).astype(BF16)
        d_gate = (d_act * lin * (sig + silu * (1.0 - sig))).astype(BF16)
        dg_ref[at, :] = d_gate
        dl_ref[at, :] = d_lin
        out_acc[at, :] += dot_nt(act, w2) if w2_turned else dot_nn(act, w2)
        back_acc[at, :] += dot_nt(d_gate, w1_ref[:]) + dot_nt(d_lin, w3_ref[:])
        return carry

    lax.fori_loop(0, rows_ref.shape[0] // chunk, step, 0)


def row_grads(lhs_s, grad, away, near, x_first):
    for slot in range(2):
        away[slot] = dot_nn(lhs_s[2 * slot + 1 if x_first else slot + 2], grad[:])
        near[slot] = dot_nn(lhs_s[2 * slot if x_first else slot], grad[:])


def expert_kernel(half, info, rows_ref, dd_ref, rows_t_ref, dd_t_ref, *refs):
    up_refs, down_refs, refs = refs[:8], refs[8:16], refs[16:]
    if half == 1:
        acc_in, refs = refs[:2], refs[2:]
    out_ref, back_ref, g1_away, g1_near, g3_away, g3_near, g2_away, g2_near, g2_rest = refs[:9]
    w1, w3, w2, act_s, dg_s, dl_s, out_acc, back_acc, lhs_s, sems = refs[9:]
    step, me = pl.program_id(0), info[0]
    same_y = (me // 2) == half
    pieces = [down_refs[2 * rel:2 * rel + 2] for rel in range(QUAD)]
    w2_halves = [w2.at[pl.ds(part * 384, 384)] for part in range(2)]
    for rel, srcs in enumerate(pieces):
        @pl.when(jnp.logical_and(same_y == (rel < 2), (step == 0) == (rel % 2 == 1)))
        def _(srcs=srcs):
            for part, src in enumerate(srcs):
                pltpu.make_async_copy(src, w2_halves[part], sems.at[part]).start()

    @pl.when(step == 0)
    def _():
        if half == 1:
            out_acc[:] = acc_in[0][:]
            back_acc[:] = acc_in[1][:]
        else:
            out_acc[:] = jnp.zeros_like(out_acc)
            back_acc[:] = jnp.zeros_like(back_acc)
        for rel in range(QUAD):
            lhs_s[rel] = rows_t_ref[pl.ds(pl.multiple_of((me ^ rel) * 192, 64), 192), :]

    for rel in range(QUAD):
        at = pl.ds(pl.multiple_of((me ^ rel) * 192, 64), 192)
        w1[at, :], w3[at, :] = (ref[:] for ref in up_refs[2 * rel:2 * rel + 2])

    def wait_w2(idx):
        @pl.when(idx == 0)
        def _():
            for part, src in enumerate(pieces[0]):
                pltpu.make_async_copy(src, w2_halves[part], sems.at[part]).wait()

    ffn_rows(rows_ref, dd_ref, w1, w3, w2, False, wait_w2, act_s, dg_s, dl_s, out_acc, back_acc)
    row_grads(lhs_s, dg_s, g1_away, g1_near, True)
    row_grads(lhs_s, dl_s, g3_away, g3_near, False)

    for near in range(2):
        @pl.when(step == near)
        def _(near=near, g2_ref=(g2_away, g2_near)[near]):
            half_rows = dd_t_ref.shape[0] // 2
            g2_ref[:] = dot_nn(dd_t_ref[:half_rows, :], act_s[:])
            g2_rest[near] = dot_nn(dd_t_ref[half_rows:, :], act_s[:])

    @pl.when(step == 1)
    def _():
        out_ref[:] = out_acc[:].astype(out_ref.dtype)
        back_ref[:] = back_acc[:].astype(back_ref.dtype)


def expert_half(half, rows, dd, rows_t, dd_t, up, down, acc):
    tok, dim = rows.shape
    y_me, x_me = lax.axis_index('y'), lax.axis_index('x')
    info = jnp.stack([2 * y_me + x_me, 2 * half + 1 - x_me, 2 * half + x_me]).astype(jnp.int32)
    whole, turned = fixed(tok, dim), fixed(dim, tok)

    up_spec = pl.BlockSpec((dim // QUAD, dim), lambda step, info_ref: (0, info_ref[1 + step]))
    any_spec = pl.BlockSpec(memory_space=pl.ANY)
    row_out = pl.BlockSpec((2, dim // QUAD, dim), lambda step, info_ref: (0, 0, info_ref[1 + step] - 2 * half))
    flat, pair = fixed(dim // 2, dim), fixed(2, dim // 2, dim)
    acc_type = F32 if half == 0 else BF16
    grad_shapes = ((2, dim // QUAD, 2 * dim),) * 4 + ((dim // 2, dim),) * 2 + ((2, dim // 2, dim),)
    return pl.pallas_call(
        lambda *refs: expert_kernel(half, *refs),
        grid_spec=pltpu.PrefetchScalarGridSpec(
            num_scalar_prefetch=1, grid=(2,),
            in_specs=[whole, whole, turned, turned] + [up_spec] * 8 + [any_spec] * 8 + [whole] * len(acc),
            out_specs=[whole, whole] + [row_out] * QUAD + [flat, flat, pair],
            scratch_shapes=[pltpu.VMEM((dim, dim), BF16)] * 3 + [pltpu.VMEM((tok, dim), BF16)] * 3 + [pltpu.VMEM((tok, dim), F32)] * 2 + [pltpu.VMEM((QUAD, dim // QUAD, tok), BF16), pltpu.SemaphoreType.DMA((2,))]),
        out_shape=[jax.ShapeDtypeStruct((tok, dim), acc_type)] * 2 + [jax.ShapeDtypeStruct(shape, F32) for shape in grad_shapes],
        compiler_params=pltpu.CompilerParams(vmem_limit_bytes=VMEM_LIMIT),
        cost_estimate=kernel_cost(36 * tok * dim * dim, dim * dim),
    )(info, rows, dd, rows_t, dd_t, *up, *down, *acc)


def shared_kernel(info, rows_ref, dd_ref, rows_t_ref, dd_t_ref, *refs):
    pieces, refs = [refs[8 * mat:8 * mat + 8] for mat in range(3)], refs[24:]
    out_refs, back_refs, g3_away, g3_near, g1_refs, g2_refs = refs[:2], refs[2:4], refs[4], refs[5], refs[6:10], refs[10:14]
    w1, w3, w2, act_s, dg_s, dl_s, out_acc, back_acc, lhs_s, lhs_z, dd_z = refs[14:]
    step, me, z_me = pl.program_id(0), info[0], info[1]

    def spot(rel, turn_z):
        return pl.ds(pl.multiple_of(((z_me ^ turn_z) * QUAD + (me ^ rel)) * ROWS, 16), ROWS)

    @pl.when(step == 0)
    def _():
        out_acc[:] = jnp.zeros_like(out_acc)
        back_acc[:] = jnp.zeros_like(back_acc)
        for rel in range(QUAD):
            for turn_z in range(QUAD):
                inner = slice(rel * ROWS, rel * ROWS + ROWS)
                lhs_s[rel, turn_z * ROWS:turn_z * ROWS + ROWS, :] = rows_t_ref[spot(rel, turn_z), :]
                lhs_z[turn_z, inner, :] = rows_t_ref[spot(rel, turn_z), :]
                dd_z[turn_z, inner, :] = dd_t_ref[spot(rel, turn_z), :]

    for w_ref, halves in zip((w1, w3, w2), pieces):
        for turn_z in range(QUAD):
            for rel in range(QUAD):
                w_ref[spot(rel, turn_z), :] = halves[2 * rel + turn_z // 2][turn_z % 2]

    ffn_rows(rows_ref, dd_ref, w1, w3, w2, True, None, act_s, dg_s, dl_s, out_acc, back_acc)
    row_grads(lhs_s, dl_s, g3_away, g3_near, True)
    for turn_z in range(QUAD):
        g1_refs[turn_z][:] = dot_nn(lhs_z[turn_z], dg_s[:])
        g2_refs[turn_z][:] = dot_nn(dd_z[turn_z], act_s[:])

    @pl.when(step == pl.num_programs(0) - 1)
    def _():
        for acc, halves in ((out_acc, out_refs), (back_acc, back_refs)):
            for ref, value in zip(halves, jnp.split(acc[:], 2, axis=0)):
                ref[:] = value


def shared_ffn(gate, rows, dd, rows_t, dd_t, pieces):
    tok, dim = rows.shape
    width = pieces[0].shape[2] // 3
    steps = width // dim
    info = after(jnp.stack([2 * lax.axis_index('y') + lax.axis_index('x'), lax.axis_index('z')]).astype(jnp.int32), gate)
    whole, turned, half = fixed(tok, dim), fixed(dim, tok), fixed(tok // 2, dim)
    piece_specs = [pl.BlockSpec((2, ROWS, dim), lambda step, info_ref, mat=mat: (0, 0, mat * steps + step)) for mat in range(3) for _ in pieces]
    row_out = pl.BlockSpec((2, dim // QUAD, dim), lambda step, info_ref: (0, 0, step))
    z_out = pl.BlockSpec((dim // QUAD, dim), lambda step, info_ref: (0, step))
    shapes = ((tok // 2, dim),) * QUAD + ((2, dim // QUAD, width),) * 2 + ((dim // QUAD, width),) * 8
    outs = pl.pallas_call(
        shared_kernel,
        grid_spec=pltpu.PrefetchScalarGridSpec(
            num_scalar_prefetch=1, grid=(steps,),
            in_specs=[whole, whole, turned, turned] + piece_specs,
            out_specs=[half] * QUAD + [row_out] * 2 + [z_out] * 8,
            scratch_shapes=[pltpu.VMEM((dim, dim), BF16)] * 3 + [pltpu.VMEM((tok, dim), BF16)] * 3 + [pltpu.VMEM((tok, dim), F32)] * 2 + [pltpu.VMEM((QUAD, dim // QUAD, tok), BF16)] * 3),
        out_shape=[jax.ShapeDtypeStruct(shape, F32) for shape in shapes],
        compiler_params=pltpu.CompilerParams(vmem_limit_bytes=VMEM_LIMIT),
        cost_estimate=kernel_cost(18 * tok * dim * width, dim * width),
    )(info, rows, dd, rows_t, dd_t, *(list(pieces) * 3))
    return outs[:2], outs[2:4], outs[4:6], outs[6:10], outs[10:]


def z_sum(plane):
    summed = plane[0]
    for step in Z_STEPS:
        summed = summed + z_hop(plane[step], step)
    return summed


def swap_rows(summed):
    halves = summed.reshape(summed.shape[:-2] + (2, -1, summed.shape[-1]))
    axis, c_me = halves.ndim - 3, lax.axis_index('c')
    return pick(halves, c_me, axis), hop(pick(halves, 1 - c_me, axis), 'c')


def plane_sum_values(total):
    y_me, x_me = lax.axis_index('y'), lax.axis_index('x')
    ways = tuple(zip((total[:2], total[2:]), ((2, x_me, y_me, 'x', 'y'), (1, y_me, x_me, 'y', 'x'))))
    gives = [pick(part, 1 - me_1, axis_1) for part, (axis_1, me_1, *_) in ways]

    def rest():
        planes = []
        for give, (part, (axis_1, me_1, me_2, name_1, name_2)) in zip(gives, ways):
            got, keep = hop(give, name_1), pick(part, me_1, axis_1)
            again = pick(keep, 1 - me_2, 1) + pick(got, 1 - me_2, 1)
            got_2 = hop(again, name_2)
            planes.append(pick(keep, me_2, 1) + pick(got, me_2, 1) + got_2)
        return jnp.concatenate(planes, axis=0)

    return gives, rest


def layer_step(x_in, grad_y, w_q, w_k, w_v, w_o, gamma_attn, gamma_mlp, w_router, w1_shared, w3_shared, w2_shared, w1_expert, w3_expert, w2_expert, expert_ids):
    n_batch, seq_len, model_dim = x_in.shape
    n_tok = n_batch * seq_len
    n_heads, head_dim = w_q.shape[1], w_q.shape[2]
    att_dim, att_half = n_heads * head_dim, n_heads * head_dim // 2
    n_experts = w_router.shape[1]
    ff_half = w1_shared.shape[1] // 2
    capacity = 2 * n_tok // n_experts
    n_slots = n_experts * capacity

    up_own, down_own = expert_halves(w1_expert, w3_expert, w2_expert)
    down_x, down_y = plane_near(down_own)
    up_x, up_y = plane_near(up_own)
    sh_chip = shared_chip([after(weight, *up_own) for weight in (w1_shared, w3_shared, w2_shared.T)])

    d_out = after(grad_y, sh_chip).reshape(n_tok, model_dim)
    onehot, dest_row = route_slots(expert_ids.reshape(n_tok), n_experts, capacity)
    place = (dest_row[:, None] == jnp.arange(n_slots)[None, :]).astype(BF16)

    def exchange(values):
        return lax.all_to_all(values.reshape(n_experts, capacity, model_dim), ('z', 'c'), 0, 0, tiled=True).reshape(n_slots, model_dim)

    def dispatch(values):
        return jnp.einsum('ts,td->sd', place, values, preferred_element_type=F32).astype(BF16)

    give_d = dispatch(d_out)
    d_down = exchange(give_d)
    w_q, w_k, w_v, w_o = (after(weight, sh_chip) for weight in (w_q, w_k, w_v, w_o))
    att_parts = (w_q.reshape(-1, att_dim), w_k.reshape(-1, att_dim), w_v.reshape(-1, att_dim), w_o.reshape(att_dim, -1).T)
    att_block = jnp.concatenate([part[:, :att_half] for part in att_parts] + [part[:, att_half:] for part in att_parts], axis=1)
    small = jnp.concatenate([gamma_attn.astype(F32)[:, None], gamma_mlp.astype(F32)[:, None], w_router], axis=1)
    small = jnp.pad(small, ((0, 0), (0, LANES - small.shape[1])))
    att_all, small_all = gather_weights(att_block, small)

    def far(from_x, from_y, *gates):
        return [hop(after(from_y[0], *gates), 'x'), hop(after(from_x[1], *gates), 'y')]

    down_far, up_far = far(down_x, down_y, small_all), far(up_x, up_y, small_all)
    sh_parts = [sh_chip] + [z_hop(after(sh_chip, small_all), step) for step in Z_STEPS]
    att_all, small_all = att_all.reshape(model_dim, -1), small_all.reshape(model_dim, -1)
    ga_all, gm_all, wr_all = small_all[:, 0], small_all[:, 1], small_all[:, 2:2 + n_experts]
    d_out_both = jnp.concatenate([d_out, hop(d_out, 'c')], axis=0)
    tables = rope_tables(seq_len, head_dim)

    tokens = x_in.reshape(n_tok, model_dim)
    qkv, normed1 = norm_qkv(tokens, ga_all[None, :], att_all)
    norm1_pull = jax.vjp(rms_norm, tokens, ga_all)[1]
    heads = attn_call(attn_fwd_kernel, 8, qkv, None, *tables, pair_spec(n_tok), att_dim)
    half_cols = [slice(start, start + att_half) for start in (0, att_half)]
    wot = [att_all[:, start + 3 * att_half:start + QUAD * att_half] for start in (0, QUAD * att_half)]
    attn_out = sum(jnp.einsum('tk,dk->td', heads[:, cols], w_half, preferred_element_type=F32) for cols, w_half in zip(half_cols, wot))
    hidden = (tokens.astype(F32) + attn_out).astype(BF16)
    normed2, norm2_pull = jax.vjp(rms_norm, hidden, gm_all)
    normed2_f = normed2.astype(F32)
    logits = jnp.dot(normed2, wr_all, preferred_element_type=F32, precision=lax.Precision.HIGHEST)
    gate_val = jax.nn.sigmoid(jnp.sum(jnp.where(onehot, logits, 0.0), axis=1))
    routed_in = (gate_val[:, None] * normed2_f).astype(BF16)
    give_r = dispatch(routed_in)
    rows = exchange(give_r)
    rows_t, d_down_t = rows.T, after(d_down, give_r).T
    normed2_both = jnp.concatenate([normed2, hop(normed2, 'c')], axis=0)
    normed2_t, d_out_t = normed2_both.T, after(d_out_both, give_r).T
    sh_parts = [after(part, qkv) for part in sh_parts]
    sh_own = jnp.stack(sh_parts[:2]), jnp.stack(sh_parts[2:])
    sh_x, sh_y = plane_near(sh_own)
    sh_far = far(sh_x, sh_y, give_r, normed2_t, d_out_t, d_down_t)
    sh_pieces, up_pieces, down_pieces = ([*own, *from_x, *from_y, *diag] for own, from_x, from_y, diag in ((sh_own, sh_x, sh_y, sh_far), (up_own, up_x, up_y, up_far), (down_own, down_x, down_y, down_far)))
    *acc, a1_away, a1_near, a3_away, a3_near, a2_away, a2_near, a2_rest = expert_half(0, rows, d_down, rows_t, d_down_t, up_pieces, down_pieces, ())
    down_rows, d_rows, b1_away, b1_near, b3_away, b3_near, b2_away, b2_near, b2_rest = expert_half(1, rows, d_down, rows_t, d_down_t, up_pieces, down_pieces, acc)
    low_y = lax.axis_index('y') == 0
    rest_got = hop(jnp.where(low_y, b2_rest, a2_rest), 'y')
    d_back = exchange(d_rows)
    back_rows = exchange(down_rows)
    shared_part, d_part, (s3_away, s3_near), s1, s2 = shared_ffn(d_rows, normed2_both, d_out_both, normed2_t, d_out_t, sh_pieces)
    shared_out = shared_part[0] + hop(shared_part[1], 'c')
    d_normed2 = d_part[0] + hop(d_part[1], 'c')


    def first_sum(away, near, axis):
        got = hop(away, axis)
        give = near[1] + got[1]
        return near[0] + got[0], hop(give, 'y' if axis == 'x' else 'x')

    a1 = first_sum(a1_away, a1_near, 'x')

    d_routed_in = jnp.einsum('ts,sd->td', place, d_back, preferred_element_type=F32)
    d_normed2 = d_normed2 + gate_val[:, None] * d_routed_in
    d_gate_val = jnp.sum(d_routed_in * normed2_f, axis=1) * gate_val * (1.0 - gate_val)
    d_logits = jnp.where(onehot, d_gate_val[:, None], 0.0)
    g_wr = jnp.einsum('td,te->de', normed2_f, d_logits, precision=lax.Precision.HIGHEST)
    d_normed2 = d_normed2 + jnp.einsum('te,de->td', d_logits, wr_all, precision=lax.Precision.HIGHEST)
    d_hid_norm, g_gm = norm2_pull(d_normed2.astype(BF16))
    d_hidden = (d_out.astype(F32) + d_hid_norm.astype(F32)).astype(BF16)

    d_hidden_t, normed1_t = d_hidden.T, normed1.T
    d_heads = jnp.concatenate([dot32(d_hidden, w_half).astype(BF16) for w_half in wot], axis=1)
    d_qkv = attn_call(attn_bwd_kernel, 16, qkv, d_heads, *tables, fixed(n_tok, 3 * att_dim), 3 * att_dim)
    d_halves = jnp.split(d_qkv, 2, axis=1)
    d_normed1 = sum(jnp.einsum('tk,dk->td', half, att_all[:, start:start + 3 * att_half], preferred_element_type=F32) for half, start in zip(d_halves, (0, QUAD * att_half)))
    d_tok_norm, g_ga = norm1_pull(d_normed1.astype(BF16))
    g_small = jnp.concatenate([g_ga[:, None], g_gm[:, None], g_wr, jnp.zeros((model_dim, 6), F32)], axis=1)
    core_0 = lax.axis_index('c') == 0

    def core_pick(pair):
        first, second = pair
        return jnp.where(core_0, first, second), jnp.where(core_0, second, first)

    g_att = []
    for lhs_t, pair in ((normed1_t, d_halves), (d_hidden_t, [heads[:, cols] for cols in half_cols])):
        mine, other = core_pick(pair)
        g_att.append(dot32(lhs_t, mine) + hop(dot32(lhs_t, other), 'c'))
    mine, other = (jnp.pad(half, ((0, 0), (0, LANES - half.shape[1]))) for half in core_pick(jnp.split(g_small, 2, axis=1)))
    g_att.append(mine + hop(other, 'c'))
    att_gives, att_rest = plane_sum_values(jnp.concatenate(g_att, axis=1).reshape(QUAD, 2, 2, ROWS, -1))

    g2_low, g2_high = a2_near + hop(a2_away, 'x'), b2_near + hop(b2_away, 'x')
    g2_give = jnp.where(low_y, g2_high, g2_low)
    rest_away, rest_near = jnp.where(low_y, a2_rest, b2_rest) + rest_got
    s3, a3 = first_sum(s3_away, s3_near, 'x'), first_sum(a3_away, a3_near, 'y')
    b3, b1 = first_sum(b3_away, b3_near, 'y'), first_sum(b1_away, b1_near, 'x')

    def finish(pair):
        mine, got = pair
        return mine + got

    def rows_by_expert(pairs):
        both = jnp.stack([finish(pair) for pair in pairs])
        halves = both.reshape(2, 2, both.shape[1] // 2, -1)
        give = pick(halves, 1 - lax.axis_index('c'), 1)
        return in_core_order(pick(halves, lax.axis_index('c'), 1)[None], hop(give, 'c')[None], 0)

    g2_full = jnp.concatenate([jnp.where(low_y, g2_low, g2_high) + hop(g2_give, 'y'), rest_near + hop(rest_away, 'x')], axis=0)
    g2_mine, g2_other = core_halves(g2_full, 1)
    g_up = jnp.concatenate([rows_by_expert((a1, a3)), rows_by_expert((b1, b3))], axis=-1)
    att_plane = att_rest()

    def z_first(parts):
        total = parts[0]
        for step in Z_STEPS:
            total = total + z_hop(parts[step], step)
        keep, give = jnp.split(total.reshape(2, 2, ROWS, -1), 2, axis=1)
        keep, give = keep + hop(give, 'x')
        return (keep + hop(give, 'y')).reshape(ROWS, -1)

    z_me = lax.axis_index('z')
    att_planes = [pick(att_plane, z_me ^ step, 0) for step in range(QUAD)]
    g_att_mine, g_att_other = swap_rows(z_sum(att_planes))
    g_sh = jnp.concatenate([z_first(s1), z_sum(finish(s3).reshape(QUAD, ROWS, -1)), z_first(s2)], axis=1)
    g_sh_mine, g_sh_other = swap_rows(g_sh)
    g_w2e = in_core_order(g2_mine.T[None], hop(g2_other, 'c').T[None], 0)
    routed = jnp.einsum('ts,sd->td', place, after(back_rows, *att_gives), preferred_element_type=F32)
    layer_out = (hidden.astype(F32) + routed + shared_out).astype(BF16)
    d_x = (d_hidden.astype(F32) + d_tok_norm.astype(F32)).astype(BF16).reshape(n_batch, seq_len, model_dim)

    g_small = in_core_order(*(part[:, QUAD * att_half:QUAD * att_half + 8] for part in (g_att_mine, g_att_other)), 1)
    g_att_mine, g_att_other = g_att_mine[:, :QUAD * att_half], g_att_other[:, :QUAD * att_half]
    g_att = in_core_order(g_att_mine.reshape(-1, QUAD, att_half), g_att_other.reshape(-1, QUAD, att_half), 2)
    g_q, g_k, g_v = (g_att[:, part].reshape(-1, n_heads, head_dim) for part in range(3))
    g_wo = g_att[:, 3].T.reshape(n_heads, head_dim, -1)
    g_sh = in_core_order(g_sh_mine.reshape(-1, 3, ff_half), g_sh_other.reshape(-1, 3, ff_half), 2)
    return (layer_out.reshape(n_batch, seq_len, model_dim), d_x, g_q, g_k, g_v, g_wo, g_small[:, 0], g_small[:, 1], g_small[:, 2:2 + n_experts], g_sh[:, 0], g_sh[:, 1], g_sh[:, 2].T, g_up[:, 0], g_up[:, 1], g_w2e)


def solution(mesh):
    fine_mesh = Mesh(np.asarray(mesh.devices).reshape(4, 2, 2, 2), AXES)
    row_spec, wo_spec, w2s_spec, exp_spec = P(AXES), P(None, None, AXES), P(None, AXES), P('z', AXES[1:])
    weight_specs = (row_spec,) * 3 + (wo_spec,) + (row_spec,) * 5 + (w2s_spec,) + (exp_spec,) * 3
    out_specs = (row_spec, row_spec) + weight_specs
    in_specs = out_specs + (row_spec,)
    return jax.shard_map(layer_step, mesh=fine_mesh, in_specs=in_specs, out_specs=out_specs, check_vma=False)
```
